32 devices in a mesh: band: 16 (over z, y, core), sub: 2 (over x).
Axes of the slice: x: 2, y: 2, z: 4, core: 2. Of those that a mesh axis runs over, the one named last changes fastest.
Arguments:
- land_values: bfloat16 [64, 524288], P(None, ('band', 'sub')), may hold values from -6 to 6
- area_weights: bfloat16 [4096, 128, 128], P(('band', 'sub')), may hold values from 0.0019989014 to 0.029907227
- land_mask: int32 [524288], P(('band', 'sub')), may hold values 0 or 1
- dest_band: int32 [4096, 1], P(('band', 'sub')), may hold values from 0 to 15; in each aligned block of 128 rows (0 to 127, 128 to 255, ...) at most 16 rows name the same one
- dest_tile: int32 [4096], P(('band', 'sub')), may hold values from 0 to 399
- ocean_mask: int32 [819200], P(('band', 'sub')), may hold values 0 or 1
Outputs:
- remapped: float32 [64, 819200], P(None, ('band', 'sub'))
The draws below stay inside these ranges and needn't reach their ends.
Inputs may be any that keep to these rules, and one draw needn't show every extreme that they name: `dest_band`: each device's 128 blocks name any one band at most 16 times; in every draw some device names one band exactly 16 times.
All inputs are finite; a program needn't handle non-finite values. No bound on the sum of `land_mask` or of `ocean_mask` on one device may be relied on, other than what follows from the above.
Results may differ from the reference program's by a relative error of at most 0.005.
Values may be sent and summed in bfloat16 or wider, within the bound.
A program may use at most 128 MiB of HBM per device.

```python
import math
import jax
import jax.numpy as jnp
import numpy as np
from jax import lax

F = 64
BL = 128
OT = 128
LB_DEV = 128
CAP = 16
TILES_BAND = 400
NBLK = 4096
NLAND = 524288
NOCN = 819200
N_BAND = 16


def touch_ends(result, rng, low, largest):
    longest = result.shape.index(max(result.shape))
    spots = []
    for shift in (0, 1):
        where = [jax.random.randint(jax.random.fold_in(rng, axis), (), 0, length) for axis, length in enumerate(result.shape)]
        where[longest] = (where[longest] + shift) % result.shape[longest]
        spots.append(tuple(where))
    return result.at[spots[0]].set(low).at[spots[1]].set(largest)


def level_of(stream_key, shape, split, least, largest):
    def one(position, shards_of):
        draws = jax.random.uniform(jax.random.fold_in(jax.random.fold_in(stream_key, 6), position), (shards_of,), jnp.float32, least / len(split), largest / len(split))
        return jnp.repeat(jnp.exp(draws), shape[position] // shards_of).reshape((-1,) + (1,) * (len(shape) - position - 1))

    gain = one(*split[0])
    for cut in split[1:]:
        gain = gain * one(*cut)
    return gain


def shared_out(own_key, own, number, rows, number_of, top, bound, lean):
    sequence = jax.random.permutation(own_key, number_of)
    packed, common = load_shares(number_of, rows * top, bound, lean, True), load_shares(number_of, rows * top, bound, lean, False)
    places = jnp.arange(number_of)

    def named(tallies, offset_by):
        used = int((tallies > 0).sum())
        fixed = max(1, used // 4)
        shifted = fixed + (places - fixed + offset_by * (used - fixed)) % max(1, number_of - fixed)
        return jnp.zeros((number_of,), jnp.int32).at[sequence[jnp.where(places < fixed, places, shifted)]].set(jnp.asarray(tallies, jnp.int32))

    tallies = jnp.where(number % 4 == 0, named(packed, number // 4), named(common, number - number // 4 - 1))
    mixed = jax.random.permutation(jax.random.fold_in(own, 3), number_of)
    donor, sink = mixed[0:number_of // 2 * 2:2], mixed[1:number_of // 2 * 2:2]
    room = jnp.minimum(tallies[donor] - 1, bound - tallies[sink]) // 2
    room = jnp.where((donor == sequence[0]) | (sink == sequence[0]) | (tallies[sink] == 0), 0, jnp.maximum(room, 0))
    shifted = jax.random.randint(jax.random.fold_in(own, 4), (number_of // 2,), 0, 1 << 20) % (room + 1)
    tallies = tallies.at[donor].add(-shifted).at[sink].add(shifted)
    labels = jnp.searchsorted(jnp.cumsum(tallies), jnp.arange(rows * top), side="right").astype(jnp.int32)
    listing = labels.reshape(top, rows).T
    listing = listing[jax.random.permutation(jax.random.fold_in(own, 1), rows)]
    offset_by = jax.random.randint(jax.random.fold_in(own, 2), (rows, 1), 0, top)
    return jnp.take_along_axis(listing, (jnp.arange(top)[None, :] + offset_by) % top, axis=1)


def load_shares(count, total, reach, lean, full):
    loads = [(1 << 20) // math.isqrt(rank ** lean) + 1 for rank in range(1, count + 1)]
    largest = reach if full else min(reach, max(-(-total // count), total * loads[0] // sum(loads)))
    least = 1 if total - largest >= count - 1 else 0
    given, surplus = [largest] + [least] * (count - 1), total - largest - least * (count - 1)
    while surplus > 0:
        free = [i for i in range(1, count) if given[i] < largest] or [i for i in range(1, count) if given[i] < reach]
        pool, budget = sum([loads[i] for i in free]), surplus
        for i in free:
            more = min(reach - given[i], max(1, budget * loads[i] // pool), surplus)
            given[i] = given[i] + more
            surplus = surplus - more
    return np.array(given)


def gaussian(stream_key, dims, spread, most, shards=(), dtype=jnp.bfloat16):
    drawn = jax.random.normal(stream_key, dims, jnp.float32) * spread
    if len(shards) > 0:
        drawn = level_of(stream_key, dims, shards, -0.22, 0.18) * drawn
    return jnp.clip(drawn, min=-most, max=most).astype(dtype)


def setup_inputs(seed: int = 0) -> dict:
    key_of = jax.random.split(jax.random.key(seed), 7)
    land_values = gaussian(key_of[0], (F, NLAND), 1.0, 6.0, ((1, 32),))
    area_weights = jnp.clip(jnp.exp(math.log(0.029907227) - 2.7055024 * jax.random.uniform(key_of[1], (NBLK, BL, OT), jnp.float32) ** level_of(key_of[1], (NBLK, BL, OT), ((0, 32),), -0.2, 0.2)), 0.0019989014, 0.029907227).astype(jnp.bfloat16)
    land_mask = touch_ends((jax.random.randint(key_of[2], (NLAND,), 0, 2) < 1).astype(jnp.int32), jax.random.fold_in(key_of[2], 1), 0, 1)
    dest_band_keys = jax.random.split(jax.random.fold_in(key_of[3], 1), NBLK // LB_DEV)
    dest_band_turns = jax.random.permutation(jax.random.fold_in(key_of[3], 3), NBLK // LB_DEV)
    dest_band = jax.vmap(lambda own, number: shared_out(jax.random.fold_in(key_of[3], 2), own, number, LB_DEV, N_BAND, 1, CAP, 2))(dest_band_keys, dest_band_turns).reshape((NBLK, 1))
    dest_tile = touch_ends(jax.random.randint(key_of[4], (NBLK,), 0, TILES_BAND), jax.random.fold_in(key_of[4], 1), 0, TILES_BAND - 1).astype(jnp.int32)
    ocean_mask = touch_ends((jax.random.randint(key_of[5], (NOCN,), 0, 4) < 3).astype(jnp.int32), jax.random.fold_in(key_of[5], 1), 0, 1)
    return dict(land_values=land_values, area_weights=area_weights, land_mask=land_mask, dest_band=dest_band, dest_tile=dest_tile, ocean_mask=ocean_mask)


cover_floor = 0.5


def reference(land_values, area_weights, land_mask, dest_band, dest_tile, ocean_mask):
    groups = area_weights.shape[0] // LB_DEV
    tiles_all = N_BAND * TILES_BAND
    block_values = land_values.reshape(F, groups, LB_DEV, BL).transpose(1, 2, 0, 3)
    block_weights = area_weights.reshape(groups, LB_DEV, BL, OT)
    block_masks = land_mask.reshape(groups, LB_DEV, BL)
    block_tiles = (dest_band[:, 0] * TILES_BAND + dest_tile).astype(jnp.int32).reshape(groups, LB_DEV)

    def remap_group(carry, inputs):
        summed, coverage = carry
        values, weights, masks, tiles = inputs
        masked = weights * masks.astype(jnp.bfloat16)[:, :, None]
        partial_value = jnp.einsum("bfl,blo->bfo", values.astype(jnp.float32), masked.astype(jnp.float32)).astype(jnp.bfloat16)
        covered = jnp.sum(masked.astype(jnp.float32), axis=1).astype(jnp.bfloat16)
        summed = summed.at[:, tiles].add(jnp.transpose(partial_value.astype(jnp.float32), (1, 0, 2)))
        coverage = coverage.at[tiles].add(covered.astype(jnp.float32))
        return (summed, coverage), None

    start_state = (jnp.zeros((F, tiles_all, OT), jnp.float32), jnp.zeros((tiles_all, OT), jnp.float32))
    (summed, coverage), unused = lax.scan(remap_group, start_state, (block_values, block_weights, block_masks, block_tiles))
    ocean_keep = ocean_mask.reshape(tiles_all, OT).astype(jnp.float32)
    remapped = summed * ocean_keep[None] / jnp.maximum(coverage, cover_floor)[None]
    return remapped.reshape(F, tiles_all * OT)
```

```python
import functools

import jax
import jax.numpy as jnp
from jax import lax
from jax.experimental import pallas as pl
from jax.experimental.pallas import tpu as pltpu
from jax.sharding import PartitionSpec as P

cover_floor = 0.5
ROWS = 8
MESH = pl.DeviceIdType.MESH
f32, bf16, i32 = jnp.float32, jnp.bfloat16, jnp.int32


def target_of(me, k, size):
    peer, bit = 0, 1
    while bit < size:
        peer = peer + bit * lax.rem(me // bit + k // bit, 2)
        bit *= 2
    return peer


def block_kernel(
    group, chunks, bands, halves, v_ref, w_ref, m_ref, t_ref, p_ref, c_ref, r_ref,
    landed, send_sem, recv_sem,
):
    band = lax.axis_index("band")
    half = lax.axis_index("sub")
    cells = w_ref.shape[1]
    everyone = bands * halves

    def peer(k):
        return {
            "band": target_of(band, k // halves, bands),
            "sub": target_of(half, lax.rem(k, halves), halves),
        }

    def index_copy(k):
        return pltpu.make_async_remote_copy(
            src_ref=t_ref, dst_ref=landed.at[k],
            send_sem=send_sem.at[k], recv_sem=recv_sem.at[k],
            device_id=peer(k), device_id_type=MESH,
        )

    @pl.when(pl.program_id(0) == 0)
    def _():
        barrier = pltpu.get_barrier_semaphore()

        @pl.loop(1, everyone)
        def _(k):
            pl.semaphore_signal(barrier, inc=1, device_id=peer(k), device_id_type=MESH)

        pl.semaphore_wait(barrier, everyone - 1)

        @pl.loop(1, everyone)
        def _(k):
            index_copy(k).start()

    for j in range(group):
        lanes = pl.ds(j * cells, cells)
        mb = m_ref[:, lanes].astype(f32).astype(bf16)
        lhs = jnp.concatenate(
            [v_ref[:, lanes] * mb, jnp.broadcast_to(mb, (16, cells))], axis=0
        )
        p = jnp.dot(lhs, w_ref[j], preferred_element_type=f32)
        for c in range(chunks):
            p_ref[c, j] = p[c * ROWS:(c + 1) * ROWS].astype(bf16)
        c_ref[pl.ds(j, 1), :] = p[chunks * ROWS:chunks * ROWS + 1].astype(bf16).astype(f32)

    @pl.when(pl.program_id(0) == pl.num_programs(0) - 1)
    def _():
        @pl.loop(1, everyone)
        def _(k):
            index_copy(k).wait_send()
            index_copy(k).wait_recv()

        r_ref[0] = t_ref[...]
        r_ref[pl.ds(1, everyone - 1)] = landed[pl.ds(1, everyone - 1)]


def block_products(bands, halves, values, weights, mask, owners):
    fields = values.shape[0]
    blocks, cells, out_cells = weights.shape
    chunks = fields // ROWS
    group = 16
    everyone = bands * halves
    return pl.pallas_call(
        functools.partial(block_kernel, group, chunks, bands, halves),
        grid=(blocks // group,),
        in_specs=[
            pl.BlockSpec((fields, group * cells), lambda i: (0, i)),
            pl.BlockSpec((group, cells, out_cells), lambda i: (i, 0, 0)),
            pl.BlockSpec((1, group * cells), lambda i: (0, i)),
            pl.BlockSpec(memory_space=pltpu.VMEM),
        ],
        out_specs=[
            pl.BlockSpec((chunks, group, ROWS, out_cells), lambda i: (0, i, 0, 0)),
            pl.BlockSpec((group, out_cells), lambda i: (i, 0)),
            pl.BlockSpec(memory_space=pltpu.VMEM),
        ],
        out_shape=[
            jax.ShapeDtypeStruct((chunks, blocks, ROWS, out_cells), bf16),
            jax.ShapeDtypeStruct((blocks, out_cells), f32),
            jax.ShapeDtypeStruct((everyone, 1, blocks), i32),
        ],
        scratch_shapes=[
            pltpu.VMEM((everyone, 1, blocks), i32),
            pltpu.SemaphoreType.DMA((everyone,)),
            pltpu.SemaphoreType.DMA((everyone,)),
        ],
        compiler_params=pltpu.CompilerParams(collective_id=1, has_side_effects=True),
        name="block_products",
    )(values, weights, mask, owners)


def exchange_kernel(
    shape, src1_ref, src2_ref, p_ref, c_ref, out_ref, cout_ref, *scratch
):
    bands, halves, planes, own, first, second, chunks = shape
    wide = bands // planes
    inside = wide * halves
    send1, send2, csend1, crecv1, cheld, csend2, cstage = scratch[:7]
    sem1, rem1, sem2, rem2, csem1, crem1, csem2, crem2, lsem, clsem = scratch[7:17]
    recv1 = scratch[17:]
    band = lax.axis_index("band")
    half = lax.axis_index("sub")

    def z_peer(k):
        return {"band": target_of(band, k * wide, bands)}

    def plane_peer(k):
        return {
            "band": target_of(band, k // halves, bands),
            "sub": target_of(half, lax.rem(k, halves), halves),
        }

    barrier = pltpu.get_barrier_semaphore()

    @pl.loop(1, planes)
    def _(k):
        pl.semaphore_signal(barrier, inc=1, device_id=z_peer(k), device_id_type=MESH)

    @pl.loop(1, inside)
    def _(k):
        pl.semaphore_signal(barrier, inc=1, device_id=plane_peer(k), device_id_type=MESH)

    pl.semaphore_wait(barrier, planes + inside - 2)

    def z_copy(c, k):
        return pltpu.make_async_remote_copy(
            src_ref=send1.at[c, k],
            dst_ref=recv1[c].at[pl.ds(own + (k - 1) * first, first)],
            send_sem=sem1.at[c, k], recv_sem=rem1.at[c, k],
            device_id=z_peer(k), device_id_type=MESH,
        )

    def plane_copy(c, k):
        return pltpu.make_async_remote_copy(
            src_ref=send2.at[c, k], dst_ref=out_ref.at[c, k],
            send_sem=sem2.at[c, k], recv_sem=rem2.at[c, k],
            device_id=plane_peer(k), device_id_type=MESH,
        )

    def z_cover(k):
        return pltpu.make_async_remote_copy(
            src_ref=csend1.at[k], dst_ref=crecv1.at[k],
            send_sem=csem1.at[k], recv_sem=crem1.at[k],
            device_id=z_peer(k), device_id_type=MESH,
        )

    def plane_cover(k):
        return pltpu.make_async_remote_copy(
            src_ref=csend2.at[k], dst_ref=cout_ref.at[k],
            send_sem=csem2.at[k], recv_sem=crem2.at[k],
            device_id=plane_peer(k), device_id_type=MESH,
        )

    def local_copy(c):
        return pltpu.make_async_copy(send2.at[c, 0], out_ref.at[c, 0], lsem.at[c])

    local_cover = pltpu.make_async_copy(csend2.at[0], cout_ref.at[0], clsem)

    def send_chunk(c):
        @pl.loop(1, planes)
        def _(k):
            for j in range(first):
                send1[c, k, j] = p_ref[c, src1_ref[own + (k - 1) * first + j]]
            z_copy(c, k).start()

        for j in range(own):
            recv1[c][j] = p_ref[c, src1_ref[j]]

    def forward_chunk(c):
        @pl.loop(1, planes)
        def _(k):
            z_copy(c, k).wait_recv()

        @pl.loop(1, inside)
        def _(k):
            for j in range(second):
                send2[c, k, j] = recv1[c][src2_ref[k * second + j]]
            plane_copy(c, k).start()

        for j in range(second):
            send2[c, 0, j] = recv1[c][src2_ref[j]]
        local_copy(c).start()

    send_chunk(0)

    @pl.loop(1, planes)
    def _(k):
        for j in range(first):
            cstage[pl.ds(j, 1), :] = c_ref[pl.ds(src1_ref[own + (k - 1) * first + j], 1), :]
        csend1[k] = cstage[pl.ds(0, first), :].astype(bf16)
        z_cover(k).start()

    for j in range(own):
        cheld[pl.ds(j, 1), :] = c_ref[pl.ds(src1_ref[j], 1), :]

    for c in range(1, chunks):
        send_chunk(c)

    for c in range(chunks):
        forward_chunk(c)
        if c == 0:
            for k in range(1, planes):
                z_cover(k).wait_recv()
                cheld[pl.ds(own + (k - 1) * first, first), :] = crecv1[k].astype(f32)

            @pl.loop(0, inside)
            def _(k):
                for j in range(second):
                    cstage[pl.ds(j, 1), :] = cheld[pl.ds(src2_ref[k * second + j], 1), :]
                csend2[k] = cstage[pl.ds(0, second), :].astype(bf16)

            @pl.loop(1, inside)
            def _(k):
                plane_cover(k).start()

            local_cover.start()

    @pl.loop(1, inside)
    def _(k):
        plane_cover(k).wait_recv()
        for c in range(chunks):
            plane_copy(c, k).wait_recv()

    local_cover.wait()
    for c in range(chunks):
        local_copy(c).wait()

    @pl.loop(1, planes)
    def _(k):
        z_cover(k).wait_send()
        for c in range(chunks):
            z_copy(c, k).wait_send()

    @pl.loop(1, inside)
    def _(k):
        plane_cover(k).wait_send()
        for c in range(chunks):
            plane_copy(c, k).wait_send()


def exchange(shape, ident, src1, src2, partial, covered):
    bands, halves, planes, own, first, second, chunks = shape
    _, _, rows, cells = partial.shape
    inside = bands * halves // planes
    held = own + (planes - 1) * first
    smem = pl.BlockSpec(memory_space=pltpu.SMEM)
    vmem = pl.BlockSpec(memory_space=pltpu.VMEM)
    hbm = pl.BlockSpec(memory_space=pl.ANY)
    dma = pltpu.SemaphoreType.DMA
    return pl.pallas_call(
        functools.partial(exchange_kernel, shape),
        in_specs=[smem, smem, vmem, vmem],
        out_specs=[hbm, hbm],
        out_shape=[
            jax.ShapeDtypeStruct((chunks, inside, second, rows, cells), bf16),
            jax.ShapeDtypeStruct((inside, second, cells), bf16),
        ],
        scratch_shapes=[
            pltpu.VMEM((chunks, planes, first, rows, cells), bf16),
            pltpu.VMEM((chunks, inside, second, rows, cells), bf16),
            pltpu.VMEM((planes, first, cells), bf16),
            pltpu.VMEM((planes, first, cells), bf16),
            pltpu.VMEM((held, cells), f32),
            pltpu.VMEM((inside, second, cells), bf16),
            pltpu.VMEM((max(first, second), cells), f32),
            dma((chunks, planes)),
            dma((chunks, planes)),
            dma((chunks, inside)),
            dma((chunks, inside)),
            dma((planes,)),
            dma((planes,)),
            dma((inside,)),
            dma((inside,)),
            dma((chunks,)),
            dma,
        ] + [pltpu.VMEM((held, rows, cells), bf16) for _ in range(chunks)],
        compiler_params=pltpu.CompilerParams(
            collective_id=ident, has_side_effects=True, vmem_limit_bytes=60 * 1024 * 1024
        ),
        name="exchange",
    )(src1, src2, partial, covered)


def gather_kernel(chunks, tiles, slot_ref, r_ref, c_ref, wet_ref, out_ref, acc, cacc, done, sem):
    step = pl.program_id(0)
    second = r_ref.shape[2]
    cells = r_ref.shape[4]
    unroll = 8

    @pl.when(step == 0)
    def _():
        @pl.loop(0, tiles)
        def _(t):
            for c in range(chunks):
                acc[c, t] = jnp.zeros((ROWS, cells), f32)

        cacc[...] = jnp.zeros_like(cacc)

    @pl.loop(0, second // unroll)
    def _(g):
        cov = c_ref[0, pl.ds(pl.multiple_of(g * unroll, unroll), unroll), :].astype(f32)
        for u in range(unroll):
            j = g * unroll + u
            t = slot_ref[step * second + j]
            for c in range(chunks):
                acc[c, t] += r_ref[c, 0, j].astype(f32)
            cacc[pl.ds(t, 1), :] += cov[u:u + 1]

    @pl.when(step == pl.num_programs(0) - 1)
    def _():
        cacc[pl.ds(0, tiles), :] = wet_ref[...].astype(f32) / jnp.maximum(
            cacc[pl.ds(0, tiles), :], cover_floor
        )

        def out_copy(c):
            return pltpu.make_async_copy(
                done.at[c], out_ref.at[pl.ds(c * ROWS, ROWS), :], sem.at[c]
            )

        for c in range(chunks):
            @pl.loop(0, tiles // unroll)
            def _(g, c=c):
                for u in range(unroll):
                    t = g * unroll + u
                    lanes = pl.ds(pl.multiple_of(t * cells, cells), cells)
                    done[c, :, lanes] = acc[c, t] * cacc[pl.ds(t, 1), :]

            out_copy(c).start()

        for c in range(chunks):
            out_copy(c).wait()


def gather(slots, arrived, covers, wet):
    chunks, inside, second, rows, cells = arrived.shape
    tiles = wet.shape[0]
    return pl.pallas_call(
        functools.partial(gather_kernel, chunks, tiles),
        grid=(inside,),
        in_specs=[
            pl.BlockSpec(memory_space=pltpu.SMEM),
            pl.BlockSpec((chunks, 1, second, rows, cells), lambda i: (0, i, 0, 0, 0)),
            pl.BlockSpec((1, second, cells), lambda i: (i, 0, 0)),
            pl.BlockSpec((tiles, cells), lambda i: (0, 0)),
        ],
        out_specs=pl.BlockSpec(memory_space=pl.ANY),
        out_shape=jax.ShapeDtypeStruct((chunks * rows, tiles * cells), f32),
        scratch_shapes=[
            pltpu.VMEM((chunks, tiles + 1, rows, cells), f32),
            pltpu.VMEM((tiles + 8, cells), f32),
            pltpu.VMEM((chunks, rows, tiles * cells), f32),
            pltpu.SemaphoreType.DMA((chunks,)),
        ],
        compiler_params=pltpu.CompilerParams(vmem_limit_bytes=60 * 1024 * 1024),
        name="gather",
    )(slots, arrived, covers, wet)


def earlier(masks):
    size = masks.shape[1]
    order = jnp.arange(size, dtype=i32)
    before = (order[:, None] < order[None, :]).astype(bf16)
    return jnp.dot(masks.astype(bf16), before, preferred_element_type=f32).astype(i32)


def pick(masks, rank, room, values):
    slot = jnp.arange(room, dtype=i32)
    hit = masks[:, None, :] & (rank[:, None, :] == slot[None, :, None])
    return jnp.sum(jnp.where(hit, values, 0), axis=2)


def per_device(land_values, area_weights, land_mask, dest_band, dest_tile, ocean_mask):
    blocks = area_weights.shape[0]
    cells = area_weights.shape[2]
    chunks = land_values.shape[0] // ROWS
    bands = lax.axis_size("band")
    halves = lax.axis_size("sub")
    everyone = bands * halves
    me = lax.axis_index("band") * halves + lax.axis_index("sub")
    tiles = ocean_mask.shape[0] // cells
    cap = max(2, 2 * blocks // bands)
    planes = 2 ** ((bands.bit_length() - 1) // 2)
    wide = bands // planes
    inside = wide * halves
    shift = (tiles - 1).bit_length()

    tile = dest_band[:, 0] * (halves * tiles) + dest_tile
    owner = tile // tiles
    packed = owner * (1 << shift) + (tile - owner * tiles)

    partial, covered, landed = block_products(
        bands, halves, land_values, area_weights, land_mask[None, :], packed[None, :]
    )

    landed = landed.reshape(planes, inside, blocks)
    rel = (landed >> shift) ^ me
    local = landed & ((1 << shift) - 1)
    queue = planes * blocks

    rel_mine = rel[0, 0]
    mine = (rel_mine // inside)[None, :] == jnp.arange(planes, dtype=i32)[:, None]
    mine = jnp.pad(mine, ((0, 0), (0, queue - blocks)))
    column = rel[:, 0, :].reshape(1, queue)
    here = column < inside
    row_of = jnp.arange(queue, dtype=i32)[None, :] // blocks
    per_row = here & (row_of == jnp.arange(planes, dtype=i32)[:, None])
    to_dest = column == jnp.arange(inside, dtype=i32)[:, None]
    to_me = (rel == 0).transpose(1, 0, 2).reshape(inside, queue)
    local_of = local.transpose(1, 0, 2).reshape(inside, queue)
    ranks = earlier(jnp.concatenate([mine, per_row, to_dest, to_me], axis=0))
    rank_mine, rank_row, rank_dest, rank_me = jnp.split(
        ranks, [planes, 2 * planes, 2 * planes + inside]
    )
    rank_row = jnp.sum(jnp.where(per_row, rank_row, 0), axis=0, keepdims=True)

    source = jnp.arange(everyone, dtype=i32).reshape(planes, inside, 1)
    plane_of = (rel ^ source) // inside
    load1 = jnp.max(jnp.stack(
        [jnp.sum((plane_of == k).astype(i32), axis=2) for k in range(1, planes)]
    ))
    by_column = rel.transpose(1, 0, 2).reshape(inside, 1, queue)
    load2 = jnp.max(jnp.sum(
        (by_column == jnp.arange(everyone, dtype=i32)[None, :, None]).astype(i32), axis=2
    ))

    wet = ocean_mask.reshape(tiles, cells)
    own = min(blocks, wide * cap)
    most = min(queue, planes * cap)
    mean1 = blocks // planes
    mean2 = max(1, queue // everyone)
    rooms = [
        (min(own, 3 * mean1 // 2), min(most, 3 * mean2)),
        (min(own, 7 * mean1 // 4), min(most, 3 * mean2)),
        (own, most),
    ]

    def run(ident, first, second):
        src1 = jnp.concatenate([
            pick(mine[:1, :blocks], rank_mine[:1, :blocks], own, jnp.arange(blocks, dtype=i32))[0],
            pick(
                mine[1:, :blocks], rank_mine[1:, :blocks], first, jnp.arange(blocks, dtype=i32)
            ).reshape(-1),
        ])
        base = jnp.where(row_of == 0, 0, own + (row_of - 1) * first)
        src2 = pick(to_dest, rank_dest, second, base + rank_row).reshape(-1)
        slots = pick(to_me, rank_me, second, (local_of - tiles)[:, None, :]).reshape(-1) + tiles
        shape = (bands, halves, planes, own, first, second, chunks)
        arrived, covers = exchange(shape, ident, src1, src2, partial, covered)
        return gather(slots, arrived, covers, wet)

    fits = [(load1 <= first) & (load2 <= second) for first, second in rooms[:-1]]
    choice = len(rooms) - 1
    for n in reversed(range(len(fits))):
        choice = jnp.where(fits[n], n, choice)
    return lax.switch(
        choice, [lambda n=n: run(2 + n, *rooms[n]) for n in range(len(rooms))]
    )


def solution(mesh):
    in_specs = (
        P(None, ("band", "sub")),
        P(("band", "sub"), None, None),
        P(("band", "sub")),
        P(("band", "sub"), None),
        P(("band", "sub")),
        P(("band", "sub")),
    )
    out_specs = P(None, ("band", "sub"))
    return jax.shard_map(
        per_device, mesh=mesh, in_specs=in_specs, out_specs=out_specs, check_vma=False
    )
```

```python
import functools

import jax
import jax.numpy as jnp
from jax import lax
from jax.experimental import pallas as pl
from jax.experimental.pallas import tpu as pltpu
from jax.sharding import PartitionSpec as P

cover_floor = 0.5
ROWS = 8
MESH = pl.DeviceIdType.MESH
f32, bf16, i32 = jnp.float32, jnp.bfloat16, jnp.int32


def target_of(me, k, size):
    peer, bit = 0, 1
    while bit < size:
        peer = peer + bit * lax.rem(me // bit + k // bit, 2)
        bit *= 2
    return peer


def block_kernel(
    group, chunks, bands, halves, v_ref, w_ref, m_ref, t_ref, p_ref, c_ref, r_ref,
    landed, send_sem, recv_sem,
):
    band = lax.axis_index("band")
    half = lax.axis_index("sub")
    cells = w_ref.shape[1]
    everyone = bands * halves

    def peer(k):
        return {
            "band": target_of(band, k // halves, bands),
            "sub": target_of(half, lax.rem(k, halves), halves),
        }

    def index_copy(k):
        return pltpu.make_async_remote_copy(
            src_ref=t_ref, dst_ref=landed.at[k],
            send_sem=send_sem.at[k], recv_sem=recv_sem.at[k],
            device_id=peer(k), device_id_type=MESH,
        )

    @pl.when(pl.program_id(0) == 0)
    def _():
        barrier = pltpu.get_barrier_semaphore()

        @pl.loop(1, everyone)
        def _(k):
            pl.semaphore_signal(barrier, inc=1, device_id=peer(k), device_id_type=MESH)

        pl.semaphore_wait(barrier, everyone - 1)

        @pl.loop(1, everyone)
        def _(k):
            index_copy(k).start()

    for j in range(group):
        lanes = pl.ds(j * cells, cells)
        mb = m_ref[:, lanes].astype(f32).astype(bf16)
        lhs = jnp.concatenate(
            [v_ref[:, lanes] * mb, jnp.broadcast_to(mb, (16, cells))], axis=0
        )
        p = jnp.dot(lhs, w_ref[j], preferred_element_type=f32)
        for c in range(chunks):
            p_ref[c, j] = p[c * ROWS:(c + 1) * ROWS].astype(bf16)
        c_ref[pl.ds(j, 1), :] = p[chunks * ROWS:chunks * ROWS + 1].astype(bf16).astype(f32)

    @pl.when(pl.program_id(0) == pl.num_programs(0) - 1)
    def _():
        @pl.loop(1, everyone)
        def _(k):
            index_copy(k).wait_send()
            index_copy(k).wait_recv()

        r_ref[0] = t_ref[...]
        r_ref[pl.ds(1, everyone - 1)] = landed[pl.ds(1, everyone - 1)]


def block_products(bands, halves, values, weights, mask, owners):
    fields = values.shape[0]
    blocks, cells, out_cells = weights.shape
    chunks = fields // ROWS
    group = 16
    everyone = bands * halves
    return pl.pallas_call(
        functools.partial(block_kernel, group, chunks, bands, halves),
        grid=(blocks // group,),
        in_specs=[
            pl.BlockSpec((fields, group * cells), lambda i: (0, i)),
            pl.BlockSpec((group, cells, out_cells), lambda i: (i, 0, 0)),
            pl.BlockSpec((1, group * cells), lambda i: (0, i)),
            pl.BlockSpec(memory_space=pltpu.VMEM),
        ],
        out_specs=[
            pl.BlockSpec((chunks, group, ROWS, out_cells), lambda i: (0, i, 0, 0)),
            pl.BlockSpec((group, out_cells), lambda i: (i, 0)),
            pl.BlockSpec(memory_space=pltpu.VMEM),
        ],
        out_shape=[
            jax.ShapeDtypeStruct((chunks, blocks, ROWS, out_cells), bf16),
            jax.ShapeDtypeStruct((blocks, out_cells), f32),
            jax.ShapeDtypeStruct((everyone, 1, blocks), i32),
        ],
        scratch_shapes=[
            pltpu.VMEM((everyone, 1, blocks), i32),
            pltpu.SemaphoreType.DMA((everyone,)),
            pltpu.SemaphoreType.DMA((everyone,)),
        ],
        compiler_params=pltpu.CompilerParams(collective_id=1, has_side_effects=True),
        name="block_products",
    )(values, weights, mask, owners)


def exchange_kernel(
    shape, list_ref, p_ref, c_ref, wet_ref, out_ref, *scratch
):
    bands, halves, planes, room1, room2, first, second, chunks, tiles = shape
    wide = bands // planes
    inside = wide * halves
    cover1, cover2 = -(-first // 8) * 8, -(-second // 8) * 8
    slots = inside * room2
    send1, send2, recv2, run, done = scratch[:5]
    csend1, crecv1, cheld, csend2, crecv2, cstage, crun, factor = scratch[5:13]
    sem1, rem1, sem2, rem2, csem1, crem1, csem2, crem2, out_sem = scratch[13:22]
    recv1 = scratch[22:]
    band = lax.axis_index("band")
    half = lax.axis_index("sub")
    cells = c_ref.shape[1]
    at2 = planes * room1
    at_prev = at2 + slots
    at_last = at_prev + slots

    def z_peer(k):
        return {"band": target_of(band, k * wide, bands)}

    def plane_peer(k):
        return {
            "band": target_of(band, k // halves, bands),
            "sub": target_of(half, lax.rem(k, halves), halves),
        }

    barrier = pltpu.get_barrier_semaphore()

    @pl.loop(1, planes)
    def _(k):
        pl.semaphore_signal(barrier, inc=1, device_id=z_peer(k), device_id_type=MESH)

    @pl.loop(1, inside)
    def _(k):
        pl.semaphore_signal(barrier, inc=1, device_id=plane_peer(k), device_id_type=MESH)

    pl.semaphore_wait(barrier, planes + inside - 2)

    def z_copy(c, k):
        return pltpu.make_async_remote_copy(
            src_ref=send1.at[c, k],
            dst_ref=recv1[c].at[pl.ds(k * room1, first)],
            send_sem=sem1.at[c, k], recv_sem=rem1.at[c, k],
            device_id=z_peer(k), device_id_type=MESH,
        )

    def plane_copy(c, k):
        return pltpu.make_async_remote_copy(
            src_ref=send2.at[c, k], dst_ref=recv2.at[c, k],
            send_sem=sem2.at[c, k], recv_sem=rem2.at[c, k],
            device_id=plane_peer(k), device_id_type=MESH,
        )

    def z_cover(k):
        return pltpu.make_async_remote_copy(
            src_ref=csend1.at[k], dst_ref=crecv1.at[k],
            send_sem=csem1.at[k], recv_sem=crem1.at[k],
            device_id=z_peer(k), device_id_type=MESH,
        )

    def plane_cover(k):
        return pltpu.make_async_remote_copy(
            src_ref=csend2.at[k], dst_ref=crecv2.at[k],
            send_sem=csem2.at[k], recv_sem=crem2.at[k],
            device_id=plane_peer(k), device_id_type=MESH,
        )

    def out_copy(c):
        return pltpu.make_async_copy(
            done.at[c % 2], out_ref.at[pl.ds(c * ROWS, ROWS), :], out_sem.at[c % 2]
        )

    def each(count, body, step=16):
        @pl.loop(0, count // step)
        def _(g):
            for u in range(step):
                body(g * step + u)

        for j in range(count // step * step, count):
            body(j)

    def send_chunk(c):
        @pl.loop(1, planes)
        def _(k):
            def pack(j):
                send1[c, k, j] = p_ref[c, list_ref[k * room1 + j]]

            each(first, pack)
            z_copy(c, k).start()

        def keep(j):
            recv1[c][j] = p_ref[c, list_ref[j]]

        each(room1, keep)

    def forward_chunk(c):
        @pl.loop(1, inside)
        def _(k):
            def pack(j):
                send2[c, k, j] = recv1[c][list_ref[at2 + k * room2 + j]]

            each(second, pack)
            plane_copy(c, k).start()

    def add_chunk(c):
        run[slots] = jnp.zeros((ROWS, cells), f32)

        def own_slot(j):
            run[j] = run[list_ref[at_prev + j]] + recv1[c][list_ref[at2 + j]].astype(f32)

        each(second, own_slot)

        @pl.loop(1, inside)
        def _(k):
            plane_copy(c, k).wait_recv()

            def one(j):
                i = k * room2 + j
                run[i] = run[list_ref[at_prev + i]] + recv2[c, k, j].astype(f32)

            each(second, one)

        if c >= 2:
            out_copy(c - 2).wait()

        def finish(t):
            lanes = pl.ds(pl.multiple_of(t * cells, cells), cells)
            done[c % 2, :, lanes] = run[list_ref[at_last + t]] * factor[pl.ds(t, 1), :]

        each(tiles, finish)
        out_copy(c).start()

    def send_covers():
        @pl.loop(1, planes)
        def _(k):
            def pack(j):
                cstage[pl.ds(j, 1), :] = c_ref[pl.ds(list_ref[k * room1 + j], 1), :]

            each(first, pack)
            csend1[k] = cstage[pl.ds(0, cover1), :].astype(bf16)
            z_cover(k).start()

        def keep(j):
            cheld[pl.ds(j, 1), :] = c_ref[pl.ds(list_ref[j], 1), :]

        each(room1, keep)

    def forward_covers():
        for k in range(1, planes):
            z_cover(k).wait_recv()
            cheld[pl.ds(k * room1, cover1), :] = crecv1[k].astype(f32)

        @pl.loop(1, inside)
        def _(k):
            def pack(j):
                cstage[pl.ds(j, 1), :] = cheld[pl.ds(list_ref[at2 + k * room2 + j], 1), :]

            each(second, pack)
            csend2[k] = cstage[pl.ds(0, cover2), :].astype(bf16)
            plane_cover(k).start()

    def add_covers():
        crun[pl.ds(slots, 8), :] = jnp.zeros((8, cells), f32)

        def own_slot(j):
            crun[pl.ds(j, 1), :] = (
                crun[pl.ds(list_ref[at_prev + j], 1), :]
                + cheld[pl.ds(list_ref[at2 + j], 1), :]
            )

        each(second, own_slot)

        @pl.loop(1, inside)
        def _(k):
            plane_cover(k).wait_recv()
            cstage[pl.ds(0, cover2), :] = crecv2[k].astype(f32)

            def one(j):
                i = k * room2 + j
                crun[pl.ds(i, 1), :] = (
                    crun[pl.ds(list_ref[at_prev + i], 1), :] + cstage[pl.ds(j, 1), :]
                )

            each(second, one)

        def total(t):
            factor[pl.ds(t, 1), :] = crun[pl.ds(list_ref[at_last + t], 1), :]

        each(tiles, total)
        factor[...] = wet_ref[...].astype(f32) / jnp.maximum(factor[...], cover_floor)

    window, lag = 2, 2
    cstage[...] = jnp.zeros_like(cstage)
    send_chunk(0)
    send_covers()
    for c in range(1, min(window, chunks)):
        send_chunk(c)

    for c in range(chunks):
        @pl.loop(1, planes)
        def _(k, c=c):
            z_copy(c, k).wait_recv()

        if c + window < chunks:
            send_chunk(c + window)
        forward_chunk(c)
        if c == 0:
            forward_covers()
        if c == lag:
            add_covers()
        if c >= lag:
            add_chunk(c - lag)

    for c in range(chunks - lag, chunks):
        add_chunk(c)

    @pl.loop(1, planes)
    def _(k):
        z_cover(k).wait_send()
        for c in range(chunks):
            z_copy(c, k).wait_send()

    @pl.loop(1, inside)
    def _(k):
        plane_cover(k).wait_send()
        for c in range(chunks):
            plane_copy(c, k).wait_send()

    for c in range(chunks - 2, chunks):
        out_copy(c).wait()


def exchange(shape, ident, lists, partial, covered, wet):
    bands, halves, planes, room1, room2, first, second, chunks, tiles = shape
    _, _, rows, cells = partial.shape
    inside = bands * halves // planes
    slots = inside * room2
    cover1, cover2 = -(-first // 8) * 8, -(-second // 8) * 8
    smem = pl.BlockSpec(memory_space=pltpu.SMEM)
    vmem = pl.BlockSpec(memory_space=pltpu.VMEM)
    dma = pltpu.SemaphoreType.DMA
    return pl.pallas_call(
        functools.partial(exchange_kernel, shape),
        in_specs=[smem, vmem, vmem, vmem],
        out_specs=pl.BlockSpec(memory_space=pl.ANY),
        out_shape=jax.ShapeDtypeStruct((chunks * rows, tiles * cells), f32),
        scratch_shapes=[
            pltpu.VMEM((chunks, planes, first, rows, cells), bf16),
            pltpu.VMEM((chunks, inside, second, rows, cells), bf16),
            pltpu.VMEM((chunks, inside, second, rows, cells), bf16),
            pltpu.VMEM((slots + 1, rows, cells), f32),
            pltpu.VMEM((2, rows, tiles * cells), f32),
            pltpu.VMEM((planes, cover1, cells), bf16),
            pltpu.VMEM((planes, cover1, cells), bf16),
            pltpu.VMEM((planes * room1, cells), f32),
            pltpu.VMEM((inside, cover2, cells), bf16),
            pltpu.VMEM((inside, cover2, cells), bf16),
            pltpu.VMEM((max(cover1, cover2), cells), f32),
            pltpu.VMEM((slots + 8, cells), f32),
            pltpu.VMEM((tiles, cells), f32),
            dma((chunks, planes)),
            dma((chunks, planes)),
            dma((chunks, inside)),
            dma((chunks, inside)),
            dma((planes,)),
            dma((planes,)),
            dma((inside,)),
            dma((inside,)),
            dma((2,)),
        ] + [pltpu.VMEM((planes * room1, rows, cells), bf16) for _ in range(chunks)],
        compiler_params=pltpu.CompilerParams(
            collective_id=ident, has_side_effects=True, vmem_limit_bytes=40 * 1024 * 1024
        ),
        name="exchange",
    )(lists, partial, covered, wet)


def earlier(masks):
    size = masks.shape[1]
    order = jnp.arange(size, dtype=i32)
    before = (order[:, None] < order[None, :]).astype(bf16)
    return jnp.dot(masks.astype(bf16), before, preferred_element_type=f32).astype(i32)


def pick(masks, rank, room, values):
    slot = jnp.arange(room, dtype=i32)
    hit = masks[:, None, :] & (rank[:, None, :] == slot[None, :, None])
    return jnp.sum(jnp.where(hit, values, 0), axis=2)


def per_device(land_values, area_weights, land_mask, dest_band, dest_tile, ocean_mask):
    blocks = area_weights.shape[0]
    cells = area_weights.shape[2]
    chunks = land_values.shape[0] // ROWS
    bands = lax.axis_size("band")
    halves = lax.axis_size("sub")
    everyone = bands * halves
    me = lax.axis_index("band") * halves + lax.axis_index("sub")
    tiles = ocean_mask.shape[0] // cells
    cap = max(2, 2 * blocks // bands)
    planes = 2 ** ((bands.bit_length() - 1) // 2)
    wide = bands // planes
    inside = wide * halves
    shift = (tiles - 1).bit_length()

    tile = dest_band[:, 0] * (halves * tiles) + dest_tile
    owner = tile // tiles
    packed = owner * (1 << shift) + (tile - owner * tiles)

    partial, covered, landed = block_products(
        bands, halves, land_values, area_weights, land_mask[None, :], packed[None, :]
    )

    landed = landed.reshape(planes, inside, blocks)
    rel = (landed >> shift) ^ me
    local = landed & ((1 << shift) - 1)
    queue = planes * blocks

    rel_mine = rel[0, 0]
    mine = (rel_mine // inside)[None, :] == jnp.arange(planes, dtype=i32)[:, None]
    mine = jnp.pad(mine, ((0, 0), (0, queue - blocks)))
    column = rel[:, 0, :].reshape(1, queue)
    here = column < inside
    row_of = jnp.arange(queue, dtype=i32)[None, :] // blocks
    per_row = here & (row_of == jnp.arange(planes, dtype=i32)[:, None])
    to_dest = column == jnp.arange(inside, dtype=i32)[:, None]
    to_me = (rel == 0).transpose(1, 0, 2).reshape(inside, queue)
    local_of = local.transpose(1, 0, 2).reshape(inside, queue)
    ranks = earlier(jnp.concatenate([mine, per_row, to_dest, to_me], axis=0))
    rank_mine, rank_row, rank_dest, rank_me = jnp.split(
        ranks, [planes, 2 * planes, 2 * planes + inside]
    )
    rank_row = jnp.sum(jnp.where(per_row, rank_row, 0), axis=0, keepdims=True)

    wet = ocean_mask.reshape(tiles, cells)
    room1 = min(blocks, wide * cap)
    room2 = min(queue, planes * cap)
    slots = inside * room2
    index = jnp.arange(blocks, dtype=i32)
    src1 = pick(mine[:, :blocks], rank_mine[:, :blocks], room1, index).reshape(-1)
    src2 = pick(to_dest, rank_dest, room2, row_of * room1 + rank_row).reshape(-1)
    tile_of = pick(to_me, rank_me, room2, (local_of + 1)[:, None, :]).reshape(-1)
    slot = jnp.arange(slots, dtype=i32)
    alike = (tile_of[:, None] == tile_of[None, :]) & (slot[None, :] < slot[:, None])
    alike = alike & (tile_of[:, None] > 0)
    prev = jnp.min(jnp.where(alike, slots - 1 - slot[None, :], slots), axis=1)
    prev = jnp.where(prev == slots, slots, slots - 1 - prev)
    listed = jnp.arange(tiles, dtype=i32) + 1
    hit = listed[:, None] == tile_of[None, :]
    last = jnp.min(jnp.where(hit, slots - 1 - slot[None, :], slots), axis=1)
    last = jnp.where(last == slots, slots, slots - 1 - last)
    lists = jnp.concatenate([src1, src2, prev, last])

    mean1 = blocks // planes
    mean2 = max(1, queue // everyone)
    rooms = [
        (min(room1, a * mean1 // 16), min(room2, b * mean2 // 16))
        for a, b in ((22, 44), (24, 44), (25, 46), (26, 48), (28, 48))
    ] + [(room1, room2)]

    source = jnp.arange(everyone, dtype=i32).reshape(planes, inside, 1)
    plane_of = ((rel ^ source) // inside).reshape(1, everyone, blocks)
    others = jnp.arange(1, planes, dtype=i32)[:, None, None]
    load1 = jnp.sum((plane_of == others).astype(i32), axis=2).reshape(-1)
    by_column = rel.transpose(1, 0, 2).reshape(inside, 1, queue)
    owners = jnp.arange(everyone, dtype=i32)[None, :, None]
    load2 = jnp.sum((by_column == owners).astype(i32), axis=2).reshape(-1)
    need1 = sum((load1 > a).astype(i32) for a, _ in rooms[:-1])
    need2 = sum((load2 > b).astype(i32) for _, b in rooms[:-1])
    choice = jnp.max(jnp.concatenate([need1, need2]))

    def run(n):
        shape = (bands, halves, planes, room1, room2, *rooms[n], chunks, tiles)
        return exchange(shape, 2 + n, lists, partial, covered, wet)

    return lax.switch(choice, [functools.partial(run, n) for n in range(len(rooms))])


def solution(mesh):
    in_specs = (
        P(None, ("band", "sub")),
        P(("band", "sub"), None, None),
        P(("band", "sub")),
        P(("band", "sub"), None),
        P(("band", "sub")),
        P(("band", "sub")),
    )
    out_specs = P(None, ("band", "sub"))
    return jax.shard_map(
        per_device, mesh=mesh, in_specs=in_specs, out_specs=out_specs, check_vma=False
    )
```

```python
import functools

import jax
import jax.numpy as jnp
from jax import lax
from jax.experimental import pallas as pl
from jax.experimental.pallas import tpu as pltpu
from jax.sharding import PartitionSpec as P

cover_floor = 0.5
ROWS = 8
MESH = pl.DeviceIdType.MESH
f32, bf16, i32 = jnp.float32, jnp.bfloat16, jnp.int32


def target_of(me, k, size):
    peer, bit = 0, 1
    while bit < size:
        peer = peer + bit * lax.rem(me // bit + k // bit, 2)
        bit *= 2
    return peer


def block_kernel(
    group, chunks, bands, halves, tiles, shift,
    v_ref, w_ref, m_ref, band_ref, tile_ref, p_ref, c_ref, r_ref,
    values, weights, named, landed, v_sem, w_sem, send_sem, recv_sem,
):
    band = lax.axis_index("band")
    half = lax.axis_index("sub")
    blocks, cells, _ = weights.shape
    everyone = bands * halves
    pieces = blocks // group

    def value_copy(i):
        lanes = pl.ds(pl.multiple_of(i * group * cells, cells), group * cells)
        return pltpu.make_async_copy(v_ref.at[:, lanes], values.at[:, lanes], v_sem.at[i])

    def weight_copy(i):
        rows = pl.ds(i * group, group)
        return pltpu.make_async_copy(w_ref.at[rows], weights.at[rows], w_sem.at[i])

    for i in range(pieces):
        value_copy(i).start()
        weight_copy(i).start()

    def peer(k):
        return {
            "band": target_of(band, k // halves, bands),
            "sub": target_of(half, lax.rem(k, halves), halves),
        }

    def index_copy(k):
        return pltpu.make_async_remote_copy(
            src_ref=named, dst_ref=landed.at[k],
            send_sem=send_sem.at[k], recv_sem=recv_sem.at[k],
            device_id=peer(k), device_id_type=MESH,
        )

    barrier = pltpu.get_barrier_semaphore()

    @pl.loop(1, everyone)
    def _(k):
        pl.semaphore_signal(barrier, inc=1, device_id=peer(k), device_id_type=MESH)

    tile = tile_ref[...]
    side = jnp.zeros_like(tile)
    for h in range(1, halves):
        side = side + (tile >= h * tiles).astype(i32)
    named[...] = (band_ref[...] * halves + side) * (1 << shift) + tile - side * tiles

    def multiply(i):
        value_copy(i).wait()
        weight_copy(i).wait()
        for u in range(group):
            j = i * group + u
            lanes = pl.ds(pl.multiple_of(j * cells, cells), cells)
            mb = m_ref[:, lanes].astype(f32).astype(bf16)
            lhs = jnp.concatenate(
                [values[:, lanes] * mb, jnp.broadcast_to(mb, (16, cells))], axis=0
            )
            p = jnp.dot(lhs, weights[j], preferred_element_type=f32)
            for c in range(chunks):
                p_ref[c, j] = p[c * ROWS:(c + 1) * ROWS].astype(bf16)
            c_ref[pl.ds(j, 1), :] = p[chunks * ROWS:chunks * ROWS + 1].astype(bf16).astype(f32)

    multiply(0)
    pl.semaphore_wait(barrier, everyone - 1)

    @pl.loop(1, everyone)
    def _(k):
        index_copy(k).start()

    @pl.loop(1, pieces)
    def _(i):
        multiply(i)

    @pl.loop(1, everyone)
    def _(k):
        index_copy(k).wait_send()
        index_copy(k).wait_recv()

    r_ref[0] = named[...]
    r_ref[pl.ds(1, everyone - 1)] = landed[pl.ds(1, everyone - 1)]


def block_products(bands, halves, tiles, shift, values, weights, mask, band, tile):
    fields = values.shape[0]
    blocks, cells, out_cells = weights.shape
    chunks = fields // ROWS
    group = 16
    pieces = blocks // group
    everyone = bands * halves
    vmem = pl.BlockSpec(memory_space=pltpu.VMEM)
    hbm = pl.BlockSpec(memory_space=pltpu.HBM)
    dma = pltpu.SemaphoreType.DMA
    return pl.pallas_call(
        functools.partial(block_kernel, group, chunks, bands, halves, tiles, shift),
        in_specs=[hbm, hbm, vmem, vmem, vmem],
        out_specs=[vmem, vmem, vmem],
        out_shape=[
            jax.ShapeDtypeStruct((chunks, blocks, ROWS, out_cells), bf16),
            jax.ShapeDtypeStruct((blocks, out_cells), f32),
            jax.ShapeDtypeStruct((everyone, 1, blocks), i32),
        ],
        scratch_shapes=[
            pltpu.VMEM(values.shape, bf16),
            pltpu.VMEM(weights.shape, bf16),
            pltpu.VMEM((1, blocks), i32),
            pltpu.VMEM((everyone, 1, blocks), i32),
            dma((pieces,)),
            dma((pieces,)),
            dma((everyone,)),
            dma((everyone,)),
        ],
        compiler_params=pltpu.CompilerParams(
            collective_id=1, has_side_effects=True, vmem_limit_bytes=59 * 1024 * 1024
        ),
        name="block_products",
    )(values, weights, mask, band, tile)


def exchange_kernel(
    shape, list_ref, p_ref, c_ref, wet_ref, out_ref, *scratch
):
    bands, halves, planes, room1, room2, first, second, chunks, tiles = shape
    wide = bands // planes
    inside = wide * halves
    cover1, cover2 = -(-first // 8) * 8, -(-second // 8) * 8
    slots = inside * room2
    send1, send2, recv2, run, done = scratch[:5]
    csend1, crecv1, cheld, csend2, crecv2, cstage, crun, factor = scratch[5:13]
    sem1, rem1, sem2, rem2, csem1, crem1, csem2, crem2, out_sem = scratch[13:22]
    recv1 = scratch[22:]
    band = lax.axis_index("band")
    half = lax.axis_index("sub")
    cells = c_ref.shape[1]
    at2 = planes * room1
    at_prev = at2 + slots
    at_last = at_prev + slots

    def z_peer(k):
        return {"band": target_of(band, k * wide, bands)}

    def plane_peer(k):
        return {
            "band": target_of(band, k // halves, bands),
            "sub": target_of(half, lax.rem(k, halves), halves),
        }

    barrier = pltpu.get_barrier_semaphore()

    @pl.loop(1, planes)
    def _(k):
        pl.semaphore_signal(barrier, inc=1, device_id=z_peer(k), device_id_type=MESH)

    @pl.loop(1, inside)
    def _(k):
        pl.semaphore_signal(barrier, inc=1, device_id=plane_peer(k), device_id_type=MESH)

    pl.semaphore_wait(barrier, planes + inside - 2)

    def z_copy(c, k):
        return pltpu.make_async_remote_copy(
            src_ref=send1.at[c, k],
            dst_ref=recv1[c].at[pl.ds(k * room1, first)],
            send_sem=sem1.at[c, k], recv_sem=rem1.at[c, k],
            device_id=z_peer(k), device_id_type=MESH,
        )

    def plane_copy(c, k):
        return pltpu.make_async_remote_copy(
            src_ref=send2.at[c, k], dst_ref=recv2.at[c, k],
            send_sem=sem2.at[c, k], recv_sem=rem2.at[c, k],
            device_id=plane_peer(k), device_id_type=MESH,
        )

    def z_cover(k):
        return pltpu.make_async_remote_copy(
            src_ref=csend1.at[k], dst_ref=crecv1.at[k],
            send_sem=csem1.at[k], recv_sem=crem1.at[k],
            device_id=z_peer(k), device_id_type=MESH,
        )

    def plane_cover(k):
        return pltpu.make_async_remote_copy(
            src_ref=csend2.at[k], dst_ref=crecv2.at[k],
            send_sem=csem2.at[k], recv_sem=crem2.at[k],
            device_id=plane_peer(k), device_id_type=MESH,
        )

    def out_copy(c):
        return pltpu.make_async_copy(
            done.at[c % 2], out_ref.at[pl.ds(c * ROWS, ROWS), :], out_sem.at[c % 2]
        )

    def each(count, body, step=16):
        @pl.loop(0, count // step)
        def _(g):
            for u in range(step):
                body(g * step + u)

        for j in range(count // step * step, count):
            body(j)

    def send_chunk(c):
        @pl.loop(1, planes)
        def _(k):
            def pack(j):
                send1[c, k, j] = p_ref[c, list_ref[k * room1 + j]]

            each(first, pack)
            z_copy(c, k).start()

        def keep(j):
            recv1[c][j] = p_ref[c, list_ref[j]]

        each(room1, keep)

    def forward_chunk(c):
        @pl.loop(1, inside)
        def _(k):
            def pack(j):
                send2[c, k, j] = recv1[c][list_ref[at2 + k * room2 + j]]

            each(second, pack)
            plane_copy(c, k).start()

    def add_chunk(c):
        run[slots] = jnp.zeros((ROWS, cells), f32)

        def own_slot(j):
            run[j] = run[list_ref[at_prev + j]] + recv1[c][list_ref[at2 + j]].astype(f32)

        each(second, own_slot)

        @pl.loop(1, inside)
        def _(k):
            plane_copy(c, k).wait_recv()

            def one(j):
                i = k * room2 + j
                run[i] = run[list_ref[at_prev + i]] + recv2[c, k, j].astype(f32)

            each(second, one)

        if c >= 2:
            out_copy(c - 2).wait()

        def finish(t):
            lanes = pl.ds(pl.multiple_of(t * cells, cells), cells)
            done[c % 2, :, lanes] = run[list_ref[at_last + t]] * factor[pl.ds(t, 1), :]

        each(tiles, finish)
        out_copy(c).start()

    def send_covers():
        @pl.loop(1, planes)
        def _(k):
            def pack(j):
                cstage[pl.ds(j, 1), :] = c_ref[pl.ds(list_ref[k * room1 + j], 1), :]

            each(first, pack)
            csend1[k] = cstage[pl.ds(0, cover1), :].astype(bf16)
            z_cover(k).start()

        def keep(j):
            cheld[pl.ds(j, 1), :] = c_ref[pl.ds(list_ref[j], 1), :]

        each(room1, keep)

    def forward_covers():
        for k in range(1, planes):
            z_cover(k).wait_recv()
            cheld[pl.ds(k * room1, cover1), :] = crecv1[k].astype(f32)

        @pl.loop(1, inside)
        def _(k):
            def pack(j):
                cstage[pl.ds(j, 1), :] = cheld[pl.ds(list_ref[at2 + k * room2 + j], 1), :]

            each(second, pack)
            csend2[k] = cstage[pl.ds(0, cover2), :].astype(bf16)
            plane_cover(k).start()

    def add_covers():
        crun[pl.ds(slots, 8), :] = jnp.zeros((8, cells), f32)

        def own_slot(j):
            crun[pl.ds(j, 1), :] = (
                crun[pl.ds(list_ref[at_prev + j], 1), :]
                + cheld[pl.ds(list_ref[at2 + j], 1), :]
            )

        each(second, own_slot)

        @pl.loop(1, inside)
        def _(k):
            plane_cover(k).wait_recv()
            cstage[pl.ds(0, cover2), :] = crecv2[k].astype(f32)

            def one(j):
                i = k * room2 + j
                crun[pl.ds(i, 1), :] = (
                    crun[pl.ds(list_ref[at_prev + i], 1), :] + cstage[pl.ds(j, 1), :]
                )

            each(second, one)

        def total(t):
            factor[pl.ds(t, 1), :] = crun[pl.ds(list_ref[at_last + t], 1), :]

        each(tiles, total)
        factor[...] = wet_ref[...].astype(f32) / jnp.maximum(factor[...], cover_floor)

    window, lag = 2, 2
    cstage[...] = jnp.zeros_like(cstage)
    send_chunk(0)
    send_covers()
    for c in range(1, min(window, chunks)):
        send_chunk(c)

    for c in range(chunks):
        @pl.loop(1, planes)
        def _(k, c=c):
            z_copy(c, k).wait_recv()

        if c + window < chunks:
            send_chunk(c + window)
        forward_chunk(c)
        if c == 0:
            forward_covers()
        if c == lag:
            add_covers()
        if c >= lag:
            add_chunk(c - lag)

    for c in range(chunks - lag, chunks):
        add_chunk(c)

    @pl.loop(1, planes)
    def _(k):
        z_cover(k).wait_send()
        for c in range(chunks):
            z_copy(c, k).wait_send()

    @pl.loop(1, inside)
    def _(k):
        plane_cover(k).wait_send()
        for c in range(chunks):
            plane_copy(c, k).wait_send()

    for c in range(chunks - 2, chunks):
        out_copy(c).wait()


def exchange(shape, ident, lists, partial, covered, wet):
    bands, halves, planes, room1, room2, first, second, chunks, tiles = shape
    _, _, rows, cells = partial.shape
    inside = bands * halves // planes
    slots = inside * room2
    cover1, cover2 = -(-first // 8) * 8, -(-second // 8) * 8
    smem = pl.BlockSpec(memory_space=pltpu.SMEM)
    vmem = pl.BlockSpec(memory_space=pltpu.VMEM)
    dma = pltpu.SemaphoreType.DMA
    return pl.pallas_call(
        functools.partial(exchange_kernel, shape),
        in_specs=[smem, vmem, vmem, vmem],
        out_specs=pl.BlockSpec(memory_space=pl.ANY),
        out_shape=jax.ShapeDtypeStruct((chunks * rows, tiles * cells), f32),
        scratch_shapes=[
            pltpu.VMEM((chunks, planes, first, rows, cells), bf16),
            pltpu.VMEM((chunks, inside, second, rows, cells), bf16),
            pltpu.VMEM((chunks, inside, second, rows, cells), bf16),
            pltpu.VMEM((slots + 1, rows, cells), f32),
            pltpu.VMEM((2, rows, tiles * cells), f32),
            pltpu.VMEM((planes, cover1, cells), bf16),
            pltpu.VMEM((planes, cover1, cells), bf16),
            pltpu.VMEM((planes * room1, cells), f32),
            pltpu.VMEM((inside, cover2, cells), bf16),
            pltpu.VMEM((inside, cover2, cells), bf16),
            pltpu.VMEM((max(cover1, cover2), cells), f32),
            pltpu.VMEM((slots + 8, cells), f32),
            pltpu.VMEM((tiles, cells), f32),
            dma((chunks, planes)),
            dma((chunks, planes)),
            dma((chunks, inside)),
            dma((chunks, inside)),
            dma((planes,)),
            dma((planes,)),
            dma((inside,)),
            dma((inside,)),
            dma((2,)),
        ] + [pltpu.VMEM((planes * room1, rows, cells), bf16) for _ in range(chunks)],
        compiler_params=pltpu.CompilerParams(
            collective_id=ident, has_side_effects=True, vmem_limit_bytes=40 * 1024 * 1024
        ),
        name="exchange",
    )(lists, partial, covered, wet)


def earlier(masks):
    size = masks.shape[1]
    order = jnp.arange(size, dtype=i32)
    before = (order[:, None] < order[None, :]).astype(bf16)
    return jnp.dot(masks.astype(bf16), before, preferred_element_type=f32).astype(i32)


def pick(masks, rank, room, values):
    slot = jnp.arange(room, dtype=i32)
    hit = masks[:, None, :] & (rank[:, None, :] == slot[None, :, None])
    return jnp.sum(jnp.where(hit, values, 0), axis=2)


def per_device(land_values, area_weights, land_mask, dest_band, dest_tile, ocean_mask):
    blocks = area_weights.shape[0]
    cells = area_weights.shape[2]
    chunks = land_values.shape[0] // ROWS
    bands = lax.axis_size("band")
    halves = lax.axis_size("sub")
    everyone = bands * halves
    me = lax.axis_index("band") * halves + lax.axis_index("sub")
    tiles = ocean_mask.shape[0] // cells
    cap = max(2, 2 * blocks // bands)
    planes = 2 ** ((bands.bit_length() - 1) // 2)
    wide = bands // planes
    inside = wide * halves
    shift = (tiles - 1).bit_length()

    partial, covered, landed = block_products(
        bands, halves, tiles, shift, land_values, area_weights,
        land_mask[None, :], dest_band.reshape(1, blocks), dest_tile[None, :],
    )

    landed = landed.reshape(planes, inside, blocks)
    rel = (landed >> shift) ^ me
    local = landed & ((1 << shift) - 1)
    queue = planes * blocks

    rel_mine = rel[0, 0]
    mine = (rel_mine // inside)[None, :] == jnp.arange(planes, dtype=i32)[:, None]
    mine = jnp.pad(mine, ((0, 0), (0, queue - blocks)))
    column = rel[:, 0, :].reshape(1, queue)
    here = column < inside
    row_of = jnp.arange(queue, dtype=i32)[None, :] // blocks
    per_row = here & (row_of == jnp.arange(planes, dtype=i32)[:, None])
    to_dest = column == jnp.arange(inside, dtype=i32)[:, None]
    to_me = (rel == 0).transpose(1, 0, 2).reshape(inside, queue)
    local_of = local.transpose(1, 0, 2).reshape(inside, queue)
    ranks = earlier(jnp.concatenate([mine, per_row, to_dest, to_me], axis=0))
    rank_mine, rank_row, rank_dest, rank_me = jnp.split(
        ranks, [planes, 2 * planes, 2 * planes + inside]
    )
    rank_row = jnp.sum(jnp.where(per_row, rank_row, 0), axis=0, keepdims=True)

    wet = ocean_mask.reshape(tiles, cells)
    room1 = min(blocks, wide * cap)
    room2 = min(queue, planes * cap)
    slots = inside * room2
    index = jnp.arange(blocks, dtype=i32)
    src1 = pick(mine[:, :blocks], rank_mine[:, :blocks], room1, index).reshape(-1)
    src2 = pick(to_dest, rank_dest, room2, row_of * room1 + rank_row).reshape(-1)
    tile_of = pick(to_me, rank_me, room2, (local_of + 1)[:, None, :]).reshape(-1)
    slot = jnp.arange(slots, dtype=i32)
    alike = (tile_of[:, None] == tile_of[None, :]) & (slot[None, :] < slot[:, None])
    alike = alike & (tile_of[:, None] > 0)
    prev = jnp.min(jnp.where(alike, slots - 1 - slot[None, :], slots), axis=1)
    prev = jnp.where(prev == slots, slots, slots - 1 - prev)
    listed = jnp.arange(tiles, dtype=i32) + 1
    hit = listed[:, None] == tile_of[None, :]
    last = jnp.min(jnp.where(hit, slots - 1 - slot[None, :], slots), axis=1)
    last = jnp.where(last == slots, slots, slots - 1 - last)
    lists = jnp.concatenate([src1, src2, prev, last])

    mean1 = blocks // planes
    mean2 = max(1, queue // everyone)
    rooms = [
        (min(room1, a * mean1 // 16), min(room2, b * mean2 // 16))
        for a, b in ((22, 44), (24, 44), (25, 46), (26, 48), (28, 48))
    ] + [(room1, room2)]

    source = jnp.arange(everyone, dtype=i32).reshape(planes, inside, 1)
    plane_of = ((rel ^ source) // inside).reshape(1, everyone, blocks)
    others = jnp.arange(1, planes, dtype=i32)[:, None, None]
    load1 = jnp.sum((plane_of == others).astype(i32), axis=2).reshape(-1)
    by_column = rel.transpose(1, 0, 2).reshape(inside, 1, queue)
    owners = jnp.arange(everyone, dtype=i32)[None, :, None]
    load2 = jnp.sum((by_column == owners).astype(i32), axis=2).reshape(-1)
    need1 = sum((load1 > a).astype(i32) for a, _ in rooms[:-1])
    need2 = sum((load2 > b).astype(i32) for _, b in rooms[:-1])
    choice = jnp.max(jnp.concatenate([need1, need2]))

    def run(n):
        shape = (bands, halves, planes, room1, room2, *rooms[n], chunks, tiles)
        return exchange(shape, 2 + n, lists, partial, covered, wet)

    return lax.switch(choice, [functools.partial(run, n) for n in range(len(rooms))])


def solution(mesh):
    in_specs = (
        P(None, ("band", "sub")),
        P(("band", "sub"), None, None),
        P(("band", "sub")),
        P(("band", "sub"), None),
        P(("band", "sub")),
        P(("band", "sub")),
    )
    out_specs = P(None, ("band", "sub"))
    return jax.shard_map(
        per_device, mesh=mesh, in_specs=in_specs, out_specs=out_specs, check_vma=False
    )
```

```python
import functools

import jax
import jax.numpy as jnp
import numpy as np
from jax import lax
from jax.experimental import pallas as pl
from jax.experimental.pallas import tpu as pltpu
from jax.sharding import PartitionSpec as P

cover_floor = 0.5
ROWS = 8
MESH = pl.DeviceIdType.MESH
f32, bf16, i32 = jnp.float32, jnp.bfloat16, jnp.int32


def peers_of(me, low, size):
    steps, bit = [], low
    while bit < size:
        steps.append(bit - 2 * bit * lax.rem(me // bit, 2))
        bit *= 2

    def peer(k):
        index = me
        for n, step in enumerate(steps):
            if not isinstance(k, int):
                index = index + step * lax.rem(k // 2 ** n, 2)
            elif k // 2 ** n % 2:
                index = index + step
        return index

    return peer


def block_kernel(
    group, chunks, bands, halves, tiles, shift,
    v_ref, w_ref, m_ref, band_ref, tile_ref, p_ref, c_ref, r_ref,
    values, weights, named, landed, v_sem, w_sem, send_sem, recv_sem,
):
    band = lax.axis_index("band")
    half = lax.axis_index("sub")
    blocks, cells, _ = weights.shape
    everyone = bands * halves
    pieces = blocks // group

    def value_copy(i):
        lanes = pl.ds(pl.multiple_of(i * group * cells, cells), group * cells)
        return pltpu.make_async_copy(v_ref.at[:, lanes], values.at[:, lanes], v_sem.at[i])

    def weight_copy(i):
        rows = pl.ds(i * group, group)
        return pltpu.make_async_copy(w_ref.at[rows], weights.at[rows], w_sem.at[i])

    for i in range(pieces):
        value_copy(i).start()
        weight_copy(i).start()

    band_at, half_at = peers_of(band, 1, bands), peers_of(half, 1, halves)

    def peer(k):
        return {"band": band_at(k // halves), "sub": half_at(k % halves)}

    def index_copy(k):
        return pltpu.make_async_remote_copy(
            src_ref=named, dst_ref=landed.at[k],
            send_sem=send_sem.at[k], recv_sem=recv_sem.at[k],
            device_id=peer(k), device_id_type=MESH,
        )

    barrier = pltpu.get_barrier_semaphore()
    for k in range(1, everyone):
        pl.semaphore_signal(barrier, inc=1, device_id=peer(k), device_id_type=MESH)

    tile = tile_ref[...]
    side = jnp.zeros_like(tile)
    for h in range(1, halves):
        side = side + (tile >= h * tiles).astype(i32)
    named[...] = (band_ref[...] * halves + side) * (1 << shift) + tile - side * tiles

    def multiply(i):
        value_copy(i).wait()
        weight_copy(i).wait()
        for u in range(group):
            j = i * group + u
            lanes = pl.ds(pl.multiple_of(j * cells, cells), cells)
            mb = m_ref[:, lanes].astype(f32).astype(bf16)
            lhs = jnp.concatenate(
                [values[:, lanes] * mb, jnp.broadcast_to(mb, (16, cells))], axis=0
            )
            p = jnp.dot(lhs, weights[j], preferred_element_type=f32)
            for c in range(chunks):
                p_ref[c, j] = p[c * ROWS:(c + 1) * ROWS].astype(bf16)
            c_ref[pl.ds(j, 1), :] = p[chunks * ROWS:chunks * ROWS + 1].astype(bf16).astype(f32)

    multiply(0)
    pl.semaphore_wait(barrier, everyone - 1)
    for k in range(1, everyone):
        index_copy(k).start()

    @pl.loop(1, pieces)
    def _(i):
        multiply(i)

    for k in range(1, everyone):
        index_copy(k).wait_send()
        index_copy(k).wait_recv()

    r_ref[0] = named[...]
    r_ref[pl.ds(1, everyone - 1)] = landed[pl.ds(1, everyone - 1)]


def block_products(bands, halves, tiles, shift, values, weights, mask, band, tile):
    fields = values.shape[0]
    blocks, cells, out_cells = weights.shape
    chunks = fields // ROWS
    group = 16
    pieces = blocks // group
    everyone = bands * halves
    vmem = pl.BlockSpec(memory_space=pltpu.VMEM)
    hbm = pl.BlockSpec(memory_space=pltpu.HBM)
    dma = pltpu.SemaphoreType.DMA
    return pl.pallas_call(
        functools.partial(block_kernel, group, chunks, bands, halves, tiles, shift),
        in_specs=[hbm, hbm, vmem, vmem, vmem],
        out_specs=[vmem, vmem, vmem],
        out_shape=[
            jax.ShapeDtypeStruct((chunks, blocks, ROWS, out_cells), bf16),
            jax.ShapeDtypeStruct((blocks, out_cells), f32),
            jax.ShapeDtypeStruct((everyone, 1, blocks), i32),
        ],
        scratch_shapes=[
            pltpu.VMEM(values.shape, bf16),
            pltpu.VMEM(weights.shape, bf16),
            pltpu.VMEM((1, blocks), i32),
            pltpu.VMEM((everyone, 1, blocks), i32),
            dma((pieces,)),
            dma((pieces,)),
            dma((everyone,)),
            dma((everyone,)),
        ],
        compiler_params=pltpu.CompilerParams(
            collective_id=1, has_side_effects=True, vmem_limit_bytes=59 * 1024 * 1024
        ),
        name="block_products",
    )(values, weights, mask, band, tile)


def exchange_kernel(
    shape, list_ref, p_ref, c_ref, wet_ref, out_ref, *scratch
):
    bands, halves, planes, room1, room2, firsts, second, chunks, tiles = shape
    first = max(firsts)
    wide = bands // planes
    inside = wide * halves
    cover1, cover2 = -(-first // 8) * 8, -(-second // 8) * 8
    slots = inside * room2
    send1, send2, recv2, run, done = scratch[:5]
    csend1, crecv1, cheld, csend2, crecv2, cstage, crun, factor = scratch[5:13]
    sem1, rem1, sem2, rem2, csem1, crem1, csem2, crem2, out_sem = scratch[13:22]
    recv1 = scratch[22:]
    band = lax.axis_index("band")
    half = lax.axis_index("sub")
    cells = c_ref.shape[1]
    at2 = planes * room1
    at_prev = at2 + slots
    at_last = at_prev + slots

    here = band // wide
    z_at = peers_of(here, 1, planes)
    wide_at, half_at = peers_of(band, 1, wide), peers_of(half, 1, halves)

    def z_peer(k):
        return {"band": band + (z_at(k) - here) * wide}

    def plane_peer(k):
        return {"band": wide_at(k // halves), "sub": half_at(k % halves)}

    barrier = pltpu.get_barrier_semaphore()

    @pl.loop(1, planes)
    def _(k):
        pl.semaphore_signal(barrier, inc=1, device_id=z_peer(k), device_id_type=MESH)

    @pl.loop(1, inside)
    def _(k):
        pl.semaphore_signal(barrier, inc=1, device_id=plane_peer(k), device_id_type=MESH)

    pl.semaphore_wait(barrier, planes + inside - 2)

    def z_copy(c, k, size):
        return pltpu.make_async_remote_copy(
            src_ref=send1.at[c, k, pl.ds(0, size)],
            dst_ref=recv1[c].at[pl.ds(k * room1, size)],
            send_sem=sem1.at[c, k], recv_sem=rem1.at[c, k],
            device_id=z_peer(k), device_id_type=MESH,
        )

    def each_target(body):
        for plane in range(planes):
            @pl.when(here != plane)
            def _(plane=plane):
                body(z_at(plane), firsts[plane])

    def each_source(body):
        for plane in range(planes):
            @pl.when(here == plane)
            def _(plane=plane):
                for k in range(1, planes):
                    body(k, firsts[plane])

    def plane_copy(c, k):
        return pltpu.make_async_remote_copy(
            src_ref=send2.at[c, k], dst_ref=recv2.at[c, k],
            send_sem=sem2.at[c, k], recv_sem=rem2.at[c, k],
            device_id=plane_peer(k), device_id_type=MESH,
        )

    def z_cover(k):
        return pltpu.make_async_remote_copy(
            src_ref=csend1.at[k], dst_ref=crecv1.at[k],
            send_sem=csem1.at[k], recv_sem=crem1.at[k],
            device_id=z_peer(k), device_id_type=MESH,
        )

    def plane_cover(k):
        return pltpu.make_async_remote_copy(
            src_ref=csend2.at[k], dst_ref=crecv2.at[k],
            send_sem=csem2.at[k], recv_sem=crem2.at[k],
            device_id=plane_peer(k), device_id_type=MESH,
        )

    def out_copy(c):
        return pltpu.make_async_copy(
            done.at[c % 2], out_ref.at[pl.ds(c * ROWS, ROWS), :], out_sem.at[c % 2]
        )

    def each(count, body, step=8):
        @pl.loop(0, count // step)
        def _(g):
            for u in range(step):
                body(g * step + u)

        for j in range(count // step * step, count):
            body(j)

    def send_chunk(c):
        @pl.loop(1, planes)
        def _(k):
            def pack(j):
                send1[c, k, j] = p_ref[c, list_ref[k * room1 + j]]

            each(first, pack)

        each_target(lambda k, size: z_copy(c, k, size).start())

        def keep(j):
            recv1[c][j] = p_ref[c, list_ref[j]]

        each(room1, keep)

    def forward_chunk(c):
        @pl.loop(1, inside)
        def _(k):
            def pack(j):
                send2[c, k, j] = recv1[c][list_ref[at2 + k * room2 + j]]

            each(second, pack)
            plane_copy(c, k).start()

    def add_chunk(c):
        run[slots] = jnp.zeros((ROWS, cells), f32)

        def own_slot(j):
            run[j] = run[list_ref[at_prev + j]] + recv1[c][list_ref[at2 + j]].astype(f32)

        each(second, own_slot)

        @pl.loop(1, inside)
        def _(k):
            plane_copy(c, k).wait_recv()

            def one(j):
                i = k * room2 + j
                run[i] = run[list_ref[at_prev + i]] + recv2[c, k, j].astype(f32)

            each(second, one)

        if c >= 2:
            out_copy(c - 2).wait()

        def finish(t):
            lanes = pl.ds(pl.multiple_of(t * cells, cells), cells)
            done[c % 2, :, lanes] = run[list_ref[at_last + t]] * factor[pl.ds(t, 1), :]

        each(tiles, finish)
        out_copy(c).start()

    def send_covers():
        @pl.loop(1, planes)
        def _(k):
            def pack(j):
                cstage[pl.ds(j, 1), :] = c_ref[pl.ds(list_ref[k * room1 + j], 1), :]

            each(first, pack)
            csend1[k] = cstage[pl.ds(0, cover1), :].astype(bf16)
            z_cover(k).start()

        def keep(j):
            cheld[pl.ds(j, 1), :] = c_ref[pl.ds(list_ref[j], 1), :]

        each(room1, keep)

    def forward_covers():
        for k in range(1, planes):
            z_cover(k).wait_recv()
            cheld[pl.ds(k * room1, cover1), :] = crecv1[k].astype(f32)

        @pl.loop(1, inside)
        def _(k):
            def pack(j):
                cstage[pl.ds(j, 1), :] = cheld[pl.ds(list_ref[at2 + k * room2 + j], 1), :]

            each(second, pack)
            csend2[k] = cstage[pl.ds(0, cover2), :].astype(bf16)
            plane_cover(k).start()

    def add_covers():
        crun[pl.ds(slots, 8), :] = jnp.zeros((8, cells), f32)

        def own_slot(j):
            crun[pl.ds(j, 1), :] = (
                crun[pl.ds(list_ref[at_prev + j], 1), :]
                + cheld[pl.ds(list_ref[at2 + j], 1), :]
            )

        each(second, own_slot)

        @pl.loop(1, inside)
        def _(k):
            plane_cover(k).wait_recv()
            cstage[pl.ds(0, cover2), :] = crecv2[k].astype(f32)

            def one(j):
                i = k * room2 + j
                crun[pl.ds(i, 1), :] = (
                    crun[pl.ds(list_ref[at_prev + i], 1), :] + cstage[pl.ds(j, 1), :]
                )

            each(second, one)

        def total(t):
            factor[pl.ds(t, 1), :] = crun[pl.ds(list_ref[at_last + t], 1), :]

        each(tiles, total)
        factor[...] = wet_ref[...].astype(f32) / jnp.maximum(factor[...], cover_floor)

    window, lag = 2, 2
    cstage[...] = jnp.zeros_like(cstage)
    send_chunk(0)
    send_covers()
    for c in range(1, min(window, chunks)):
        send_chunk(c)

    for c in range(chunks):
        each_source(lambda k, size: z_copy(c, k, size).wait_recv())
        if c + window < chunks:
            send_chunk(c + window)
        forward_chunk(c)
        if c == 0:
            forward_covers()
        if c == lag:
            add_covers()
        if c >= lag:
            add_chunk(c - lag)

    for c in range(chunks - lag, chunks):
        add_chunk(c)

    @pl.loop(1, planes)
    def _(k):
        z_cover(k).wait_send()

    for c in range(chunks):
        each_target(lambda k, size: z_copy(c, k, size).wait_send())

    @pl.loop(1, inside)
    def _(k):
        plane_cover(k).wait_send()
        for c in range(chunks):
            plane_copy(c, k).wait_send()

    for c in range(chunks - 2, chunks):
        out_copy(c).wait()


def exchange(shape, ident, lists, partial, covered, wet):
    bands, halves, planes, room1, room2, firsts, second, chunks, tiles = shape
    first = max(firsts)
    _, _, rows, cells = partial.shape
    inside = bands * halves // planes
    slots = inside * room2
    cover1, cover2 = -(-first // 8) * 8, -(-second // 8) * 8
    smem = pl.BlockSpec(memory_space=pltpu.SMEM)
    vmem = pl.BlockSpec(memory_space=pltpu.VMEM)
    dma = pltpu.SemaphoreType.DMA
    return pl.pallas_call(
        functools.partial(exchange_kernel, shape),
        in_specs=[smem, vmem, vmem, vmem],
        out_specs=pl.BlockSpec(memory_space=pl.ANY),
        out_shape=jax.ShapeDtypeStruct((chunks * rows, tiles * cells), f32),
        scratch_shapes=[
            pltpu.VMEM((chunks, planes, first, rows, cells), bf16),
            pltpu.VMEM((chunks, inside, second, rows, cells), bf16),
            pltpu.VMEM((chunks, inside, second, rows, cells), bf16),
            pltpu.VMEM((slots + 1, rows, cells), f32),
            pltpu.VMEM((2, rows, tiles * cells), f32),
            pltpu.VMEM((planes, cover1, cells), bf16),
            pltpu.VMEM((planes, cover1, cells), bf16),
            pltpu.VMEM((planes * room1, cells), f32),
            pltpu.VMEM((inside, cover2, cells), bf16),
            pltpu.VMEM((inside, cover2, cells), bf16),
            pltpu.VMEM((max(cover1, cover2), cells), f32),
            pltpu.VMEM((slots + 8, cells), f32),
            pltpu.VMEM((tiles, cells), f32),
            dma((chunks, planes)),
            dma((chunks, planes)),
            dma((chunks, inside)),
            dma((chunks, inside)),
            dma((planes,)),
            dma((planes,)),
            dma((inside,)),
            dma((inside,)),
            dma((2,)),
        ] + [pltpu.VMEM((planes * room1, rows, cells), bf16) for _ in range(chunks)],
        compiler_params=pltpu.CompilerParams(
            collective_id=ident, has_side_effects=True, vmem_limit_bytes=40 * 1024 * 1024
        ),
        name="exchange",
    )(lists, partial, covered, wet)


def earlier(masks):
    size = masks.shape[1]
    order = jnp.arange(size, dtype=i32)
    before = (order[:, None] < order[None, :]).astype(bf16)
    return jnp.dot(masks.astype(bf16), before, preferred_element_type=f32).astype(i32)


def pick(masks, rank, room, values):
    slot = jnp.arange(room, dtype=i32)
    hit = masks[:, None, :] & (rank[:, None, :] == slot[None, :, None])
    return jnp.sum(jnp.where(hit, values, 0), axis=2)


def per_device(land_values, area_weights, land_mask, dest_band, dest_tile, ocean_mask):
    blocks = area_weights.shape[0]
    cells = area_weights.shape[2]
    chunks = land_values.shape[0] // ROWS
    bands = lax.axis_size("band")
    halves = lax.axis_size("sub")
    everyone = bands * halves
    me = lax.axis_index("band") * halves + lax.axis_index("sub")
    tiles = ocean_mask.shape[0] // cells
    cap = max(2, 2 * blocks // bands)
    planes = 2 ** ((bands.bit_length() - 1) // 2)
    wide = bands // planes
    inside = wide * halves
    shift = (tiles - 1).bit_length()

    partial, covered, landed = block_products(
        bands, halves, tiles, shift, land_values, area_weights,
        land_mask[None, :], dest_band.reshape(1, blocks), dest_tile[None, :],
    )

    landed = landed.reshape(planes, inside, blocks)
    rel = (landed >> shift) ^ me
    local = landed & ((1 << shift) - 1)
    queue = planes * blocks

    rel_mine = rel[0, 0]
    mine = (rel_mine // inside)[None, :] == jnp.arange(planes, dtype=i32)[:, None]
    mine = jnp.pad(mine, ((0, 0), (0, queue - blocks)))
    column = rel[:, 0, :].reshape(1, queue)
    here = column < inside
    row_of = jnp.arange(queue, dtype=i32)[None, :] // blocks
    per_row = here & (row_of == jnp.arange(planes, dtype=i32)[:, None])
    to_dest = column == jnp.arange(inside, dtype=i32)[:, None]
    to_me = (rel == 0).transpose(1, 0, 2).reshape(inside, queue)
    local_of = local.transpose(1, 0, 2).reshape(inside, queue)
    ranks = earlier(jnp.concatenate([mine, per_row, to_dest, to_me], axis=0))
    rank_mine, rank_row, rank_dest, rank_me = jnp.split(
        ranks, [planes, 2 * planes, 2 * planes + inside]
    )
    rank_row = jnp.sum(jnp.where(per_row, rank_row, 0), axis=0, keepdims=True)

    wet = ocean_mask.reshape(tiles, cells)
    room1 = min(blocks, wide * cap)
    room2 = min(queue, planes * cap)
    slots = inside * room2
    index = jnp.arange(blocks, dtype=i32)
    src1 = pick(mine[:, :blocks], rank_mine[:, :blocks], room1, index).reshape(-1)
    src2 = pick(to_dest, rank_dest, room2, row_of * room1 + rank_row).reshape(-1)
    tile_of = pick(to_me, rank_me, room2, (local_of + 1)[:, None, :]).reshape(-1)
    slot = jnp.arange(slots, dtype=i32)
    alike = (tile_of[:, None] == tile_of[None, :]) & (slot[None, :] < slot[:, None])
    alike = alike & (tile_of[:, None] > 0)
    prev = jnp.min(jnp.where(alike, slots - 1 - slot[None, :], slots), axis=1)
    prev = jnp.where(prev == slots, slots, slots - 1 - prev)
    listed = jnp.arange(tiles, dtype=i32) + 1
    hit = listed[:, None] == tile_of[None, :]
    last = jnp.min(jnp.where(hit, slots - 1 - slot[None, :], slots), axis=1)
    last = jnp.where(last == slots, slots, slots - 1 - last)
    lists = jnp.concatenate([src1, src2, prev, last])

    mean1 = blocks // planes
    mean2 = max(1, queue // everyone)
    sizes = [(a,) * planes for a in (44, 48)] if planes != 4 else [
        (40, 44, 40, 44), (38, 50, 50, 38), (50, 38, 38, 50),
        (44, 46, 44, 46), (40, 56, 40, 56), (56, 40, 56, 40),
    ]
    rooms = [
        (tuple(min(room1, a * mean1 // 32) for a in size), min(room2, b * mean2 // 16))
        for size, b in [(size, 44) for size in sizes]
        + [((52,) * planes, 48), ((56,) * planes, 48)]
    ] + [((room1,) * planes, room2)]

    source = jnp.arange(everyone, dtype=i32).reshape(planes, inside) ^ me
    plane_of = ((landed >> shift) // inside).reshape(1, everyone, blocks)
    target = jnp.arange(planes, dtype=i32)[:, None]
    load1 = jnp.sum((plane_of == target[:, :, None]).astype(i32), axis=2)
    load1 = jnp.where((source // inside).reshape(1, everyone) == target, 0, load1)
    by_column = rel.transpose(1, 0, 2).reshape(inside, 1, queue)
    owners = jnp.arange(everyone, dtype=i32)[None, :, None]
    load2 = jnp.sum((by_column == owners).astype(i32), axis=2)
    need1, need2 = jnp.zeros_like(load1), jnp.zeros_like(load2)
    for n, (size, b) in enumerate(rooms[:-1]):
        allowed = sum((target == p).astype(i32) * a for p, a in enumerate(size))
        need1 = need1 | ((load1 > allowed).astype(i32) << n)
        need2 = need2 | ((load2 > b).astype(i32) << n)
    need = jnp.concatenate([need1, need2]) if planes != inside else need1 | need2
    full = lax.reduce(need, np.int32(0), lax.bitwise_or, (0, 1))
    choice, still = jnp.int32(0), jnp.int32(1)
    for n in range(len(rooms) - 1):
        still = still & (full >> n)
        choice = choice + still

    def run(n):
        shape = (bands, halves, planes, room1, room2, *rooms[n], chunks, tiles)
        return exchange(shape, 2 + n, lists, partial, covered, wet)

    return lax.switch(choice, [functools.partial(run, n) for n in range(len(rooms))])


def solution(mesh):
    in_specs = (
        P(None, ("band", "sub")),
        P(("band", "sub"), None, None),
        P(("band", "sub")),
        P(("band", "sub"), None),
        P(("band", "sub")),
        P(("band", "sub")),
    )
    out_specs = P(None, ("band", "sub"))
    return jax.shard_map(
        per_device, mesh=mesh, in_specs=in_specs, out_specs=out_specs, check_vma=False
    )
```

```python
import functools

import jax
import jax.numpy as jnp
import numpy as np
from jax import lax
from jax.experimental import pallas as pl
from jax.experimental.pallas import tpu as pltpu
from jax.sharding import PartitionSpec as P

cover_floor = 0.5
ROWS = 8
MESH = pl.DeviceIdType.MESH
f32, bf16, i32 = jnp.float32, jnp.bfloat16, jnp.int32


def peers_of(me, low, size):
    steps, bit = [], low
    while bit < size:
        steps.append(bit - 2 * bit * lax.rem(me // bit, 2))
        bit *= 2

    def peer(k):
        index = me
        for n, step in enumerate(steps):
            if not isinstance(k, int):
                index = index + step * lax.rem(k // 2 ** n, 2)
            elif k // 2 ** n % 2:
                index = index + step
        return index

    return peer


def block_kernel(
    group, chunks, bands, halves, tiles, shift,
    v_ref, w_ref, m_ref, band_ref, tile_ref, p_ref, c_ref, r_ref,
    values, weights, named, landed, v_sem, w_sem, send_sem, recv_sem,
):
    band = lax.axis_index("band")
    half = lax.axis_index("sub")
    blocks, cells, _ = weights.shape
    everyone = bands * halves
    pieces = blocks // group

    def value_copy(i):
        lanes = pl.ds(pl.multiple_of(i * group * cells, cells), group * cells)
        return pltpu.make_async_copy(v_ref.at[:, lanes], values.at[:, lanes], v_sem.at[i])

    def weight_copy(i):
        rows = pl.ds(i * group, group)
        return pltpu.make_async_copy(w_ref.at[rows], weights.at[rows], w_sem.at[i])

    for i in range(pieces):
        value_copy(i).start()
        weight_copy(i).start()

    band_at, half_at = peers_of(band, 1, bands), peers_of(half, 1, halves)

    def peer(k):
        return {"band": band_at(k // halves), "sub": half_at(k % halves)}

    def index_copy(k):
        return pltpu.make_async_remote_copy(
            src_ref=named, dst_ref=landed.at[k],
            send_sem=send_sem.at[k], recv_sem=recv_sem.at[k],
            device_id=peer(k), device_id_type=MESH,
        )

    barrier = pltpu.get_barrier_semaphore()
    for k in range(1, everyone):
        pl.semaphore_signal(barrier, inc=1, device_id=peer(k), device_id_type=MESH)

    tile = tile_ref[...]
    side = jnp.zeros_like(tile)
    for h in range(1, halves):
        side = side + (tile >= h * tiles).astype(i32)
    named[...] = (band_ref[...] * halves + side) * (1 << shift) + tile - side * tiles

    def multiply(i):
        value_copy(i).wait()
        weight_copy(i).wait()
        for u in range(group):
            j = i * group + u
            lanes = pl.ds(pl.multiple_of(j * cells, cells), cells)
            mb = m_ref[:, lanes].astype(f32).astype(bf16)
            lhs = jnp.concatenate(
                [values[:, lanes] * mb, jnp.broadcast_to(mb, (16, cells))], axis=0
            )
            p = jnp.dot(lhs, weights[j], preferred_element_type=f32)
            for c in range(chunks):
                p_ref[c, j] = p[c * ROWS:(c + 1) * ROWS].astype(bf16)
            c_ref[pl.ds(j, 1), :] = p[chunks * ROWS:chunks * ROWS + 1].astype(bf16).astype(f32)

    multiply(0)
    pl.semaphore_wait(barrier, everyone - 1)
    for k in range(1, everyone):
        index_copy(k).start()

    @pl.loop(1, pieces)
    def _(i):
        multiply(i)

    for k in range(1, everyone):
        index_copy(k).wait_send()
        index_copy(k).wait_recv()

    r_ref[0] = named[...]
    r_ref[pl.ds(1, everyone - 1)] = landed[pl.ds(1, everyone - 1)]


def block_products(bands, halves, tiles, shift, values, weights, mask, band, tile):
    fields = values.shape[0]
    blocks, cells, out_cells = weights.shape
    chunks = fields // ROWS
    group = 16
    pieces = blocks // group
    everyone = bands * halves
    vmem = pl.BlockSpec(memory_space=pltpu.VMEM)
    hbm = pl.BlockSpec(memory_space=pltpu.HBM)
    dma = pltpu.SemaphoreType.DMA
    return pl.pallas_call(
        functools.partial(block_kernel, group, chunks, bands, halves, tiles, shift),
        in_specs=[hbm, hbm, vmem, vmem, vmem],
        out_specs=[vmem, vmem, vmem],
        out_shape=[
            jax.ShapeDtypeStruct((chunks, blocks, ROWS, out_cells), bf16),
            jax.ShapeDtypeStruct((blocks, out_cells), f32),
            jax.ShapeDtypeStruct((everyone, 1, blocks), i32),
        ],
        scratch_shapes=[
            pltpu.VMEM(values.shape, bf16),
            pltpu.VMEM(weights.shape, bf16),
            pltpu.VMEM((1, blocks), i32),
            pltpu.VMEM((everyone, 1, blocks), i32),
            dma((pieces,)),
            dma((pieces,)),
            dma((everyone,)),
            dma((everyone,)),
        ],
        compiler_params=pltpu.CompilerParams(
            collective_id=1, has_side_effects=True, vmem_limit_bytes=59 * 1024 * 1024
        ),
        name="block_products",
    )(values, weights, mask, band, tile)


def exchange_kernel(
    shape, list_ref, p_ref, c_ref, wet_ref, out_ref, *scratch
):
    bands, halves, planes, room1, room2, firsts, second, chunks, tiles = shape
    first = max(firsts)
    wide = bands // planes
    inside = wide * halves
    cover1, cover2 = -(-first // 8) * 8, -(-second // 8) * 8
    slots = inside * room2
    send1, send2, recv2, run, done = scratch[:5]
    csend1, crecv1, cheld, csend2, crecv2, cstage, crun, factor = scratch[5:13]
    sem1, rem1, sem2, rem2, csem1, crem1, csem2, crem2, out_sem = scratch[13:22]
    recv1 = scratch[22:]
    band = lax.axis_index("band")
    half = lax.axis_index("sub")
    cells = c_ref.shape[1]
    at2 = planes * room1
    at_prev = at2 + slots
    at_last = at_prev + slots

    here = band // wide
    z_at = peers_of(here, 1, planes)
    wide_at, half_at = peers_of(band, 1, wide), peers_of(half, 1, halves)

    def z_peer(k):
        return {"band": band + (z_at(k) - here) * wide}

    def plane_peer(k):
        return {"band": wide_at(k // halves), "sub": half_at(k % halves)}

    barrier = pltpu.get_barrier_semaphore()

    @pl.loop(1, planes)
    def _(k):
        pl.semaphore_signal(barrier, inc=1, device_id=z_peer(k), device_id_type=MESH)

    @pl.loop(1, inside)
    def _(k):
        pl.semaphore_signal(barrier, inc=1, device_id=plane_peer(k), device_id_type=MESH)

    pl.semaphore_wait(barrier, planes + inside - 2)

    def z_copy(c, k, size):
        return pltpu.make_async_remote_copy(
            src_ref=send1.at[c, k, pl.ds(0, size)],
            dst_ref=recv1[c].at[pl.ds(k * room1, size)],
            send_sem=sem1.at[c, k], recv_sem=rem1.at[c, k],
            device_id=z_peer(k), device_id_type=MESH,
        )

    def each_target(body):
        for plane in range(planes):
            @pl.when(here != plane)
            def _(plane=plane):
                body(z_at(plane), firsts[plane])

    def each_source(body):
        for plane in range(planes):
            @pl.when(here == plane)
            def _(plane=plane):
                for k in range(1, planes):
                    body(k, firsts[plane])

    def plane_copy(c, k):
        return pltpu.make_async_remote_copy(
            src_ref=send2.at[c, k], dst_ref=recv2.at[c, k],
            send_sem=sem2.at[c, k], recv_sem=rem2.at[c, k],
            device_id=plane_peer(k), device_id_type=MESH,
        )

    def z_cover(k):
        return pltpu.make_async_remote_copy(
            src_ref=csend1.at[k], dst_ref=crecv1.at[k],
            send_sem=csem1.at[k], recv_sem=crem1.at[k],
            device_id=z_peer(k), device_id_type=MESH,
        )

    def plane_cover(k):
        return pltpu.make_async_remote_copy(
            src_ref=csend2.at[k], dst_ref=crecv2.at[k],
            send_sem=csem2.at[k], recv_sem=crem2.at[k],
            device_id=plane_peer(k), device_id_type=MESH,
        )

    def out_copy(c):
        return pltpu.make_async_copy(
            done.at[c % 2], out_ref.at[pl.ds(c * ROWS, ROWS), :], out_sem.at[c % 2]
        )

    def each(count, body, step=4):
        @pl.loop(0, count // step)
        def _(g):
            for u in range(step):
                body(g * step + u)

        for j in range(count // step * step, count):
            body(j)

    def send_chunk(c):
        def to_plane(k, size):
            def pack(j):
                send1[c, k, j] = p_ref[c, list_ref[k * room1 + j]]

            each(size, pack)
            z_copy(c, k, size).start()

        each_target(to_plane)

        def keep(j):
            recv1[c][j] = p_ref[c, list_ref[j]]

        each(room1, keep)

    def forward_chunk(c):
        @pl.loop(1, inside)
        def _(k):
            def pack(j):
                send2[c, k, j] = recv1[c][list_ref[at2 + k * room2 + j]]

            each(second, pack)
            plane_copy(c, k).start()

    def add_chunk(c):
        run[slots] = jnp.zeros((ROWS, cells), f32)

        def own_slot(j):
            run[j] = run[list_ref[at_prev + j]] + recv1[c][list_ref[at2 + j]].astype(f32)

        each(second, own_slot)

        @pl.loop(1, inside)
        def _(k):
            plane_copy(c, k).wait_recv()

            def one(j):
                i = k * room2 + j
                run[i] = run[list_ref[at_prev + i]] + recv2[c, k, j].astype(f32)

            each(second, one)

        if c >= 2:
            out_copy(c - 2).wait()

        def finish(t):
            lanes = pl.ds(pl.multiple_of(t * cells, cells), cells)
            done[c % 2, :, lanes] = run[list_ref[at_last + t]] * factor[pl.ds(t, 1), :]

        each(tiles, finish)
        out_copy(c).start()

    def send_covers():
        @pl.loop(1, planes)
        def _(k):
            def pack(j):
                cstage[pl.ds(j, 1), :] = c_ref[pl.ds(list_ref[k * room1 + j], 1), :]

            each(first, pack)
            csend1[k] = cstage[pl.ds(0, cover1), :].astype(bf16)
            z_cover(k).start()

        def keep(j):
            cheld[pl.ds(j, 1), :] = c_ref[pl.ds(list_ref[j], 1), :]

        each(room1, keep)

    def forward_covers():
        for k in range(1, planes):
            z_cover(k).wait_recv()
            cheld[pl.ds(k * room1, cover1), :] = crecv1[k].astype(f32)

        @pl.loop(1, inside)
        def _(k):
            def pack(j):
                cstage[pl.ds(j, 1), :] = cheld[pl.ds(list_ref[at2 + k * room2 + j], 1), :]

            each(second, pack)
            csend2[k] = cstage[pl.ds(0, cover2), :].astype(bf16)
            plane_cover(k).start()

    def add_covers():
        crun[pl.ds(slots, 8), :] = jnp.zeros((8, cells), f32)

        def own_slot(j):
            crun[pl.ds(j, 1), :] = (
                crun[pl.ds(list_ref[at_prev + j], 1), :]
                + cheld[pl.ds(list_ref[at2 + j], 1), :]
            )

        each(second, own_slot)

        @pl.loop(1, inside)
        def _(k):
            plane_cover(k).wait_recv()
            cstage[pl.ds(0, cover2), :] = crecv2[k].astype(f32)

            def one(j):
                i = k * room2 + j
                crun[pl.ds(i, 1), :] = (
                    crun[pl.ds(list_ref[at_prev + i], 1), :] + cstage[pl.ds(j, 1), :]
                )

            each(second, one)

        def total(t):
            factor[pl.ds(t, 1), :] = crun[pl.ds(list_ref[at_last + t], 1), :]

        each(tiles, total)
        factor[...] = wet_ref[...].astype(f32) / jnp.maximum(factor[...], cover_floor)

    window, lag = 2, 1
    cstage[...] = jnp.zeros_like(cstage)
    send_chunk(0)
    send_covers()
    for c in range(1, min(window, chunks)):
        send_chunk(c)

    for c in range(chunks):
        each_source(lambda k, size: z_copy(c, k, size).wait_recv())
        forward_chunk(c)
        if c + window < chunks:
            send_chunk(c + window)
        if c == 0:
            forward_covers()
        if c == lag:
            add_covers()
        if c >= lag:
            add_chunk(c - lag)

    for c in range(chunks - lag, chunks):
        add_chunk(c)

    @pl.loop(1, planes)
    def _(k):
        z_cover(k).wait_send()

    for c in range(chunks):
        each_target(lambda k, size: z_copy(c, k, size).wait_send())

    @pl.loop(1, inside)
    def _(k):
        plane_cover(k).wait_send()
        for c in range(chunks):
            plane_copy(c, k).wait_send()

    for c in range(chunks - 2, chunks):
        out_copy(c).wait()


def exchange(shape, ident, lists, partial, covered, wet):
    bands, halves, planes, room1, room2, firsts, second, chunks, tiles = shape
    first = max(firsts)
    _, _, rows, cells = partial.shape
    inside = bands * halves // planes
    slots = inside * room2
    cover1, cover2 = -(-first // 8) * 8, -(-second // 8) * 8
    smem = pl.BlockSpec(memory_space=pltpu.SMEM)
    vmem = pl.BlockSpec(memory_space=pltpu.VMEM)
    dma = pltpu.SemaphoreType.DMA
    return pl.pallas_call(
        functools.partial(exchange_kernel, shape),
        in_specs=[smem, vmem, vmem, vmem],
        out_specs=pl.BlockSpec(memory_space=pl.ANY),
        out_shape=jax.ShapeDtypeStruct((chunks * rows, tiles * cells), f32),
        scratch_shapes=[
            pltpu.VMEM((chunks, planes, first, rows, cells), bf16),
            pltpu.VMEM((chunks, inside, second, rows, cells), bf16),
            pltpu.VMEM((chunks, inside, second, rows, cells), bf16),
            pltpu.VMEM((slots + 1, rows, cells), f32),
            pltpu.VMEM((2, rows, tiles * cells), f32),
            pltpu.VMEM((planes, cover1, cells), bf16),
            pltpu.VMEM((planes, cover1, cells), bf16),
            pltpu.VMEM((planes * room1, cells), f32),
            pltpu.VMEM((inside, cover2, cells), bf16),
            pltpu.VMEM((inside, cover2, cells), bf16),
            pltpu.VMEM((max(cover1, cover2), cells), f32),
            pltpu.VMEM((slots + 8, cells), f32),
            pltpu.VMEM((tiles, cells), f32),
            dma((chunks, planes)),
            dma((chunks, planes)),
            dma((chunks, inside)),
            dma((chunks, inside)),
            dma((planes,)),
            dma((planes,)),
            dma((inside,)),
            dma((inside,)),
            dma((2,)),
        ] + [pltpu.VMEM((planes * room1, rows, cells), bf16) for _ in range(chunks)],
        compiler_params=pltpu.CompilerParams(
            collective_id=ident, has_side_effects=True, vmem_limit_bytes=40 * 1024 * 1024
        ),
        name="exchange",
    )(lists, partial, covered, wet)


def earlier(masks):
    size = masks.shape[1]
    order = jnp.arange(size, dtype=i32)
    before = (order[:, None] < order[None, :]).astype(bf16)
    return jnp.dot(masks.astype(bf16), before, preferred_element_type=f32).astype(i32)


def pick(masks, rank, room, values):
    slot = jnp.arange(room, dtype=i32)
    hit = masks[:, None, :] & (rank[:, None, :] == slot[None, :, None])
    return jnp.sum(jnp.where(hit, values, 0), axis=2)


def per_device(land_values, area_weights, land_mask, dest_band, dest_tile, ocean_mask):
    blocks = area_weights.shape[0]
    cells = area_weights.shape[2]
    chunks = land_values.shape[0] // ROWS
    bands = lax.axis_size("band")
    halves = lax.axis_size("sub")
    everyone = bands * halves
    me = lax.axis_index("band") * halves + lax.axis_index("sub")
    tiles = ocean_mask.shape[0] // cells
    cap = max(2, 2 * blocks // bands)
    planes = 2 ** ((bands.bit_length() - 1) // 2)
    wide = bands // planes
    inside = wide * halves
    shift = (tiles - 1).bit_length()

    partial, covered, landed = block_products(
        bands, halves, tiles, shift, land_values, area_weights,
        land_mask[None, :], dest_band.reshape(1, blocks), dest_tile[None, :],
    )

    landed = landed.reshape(planes, inside, blocks)
    rel = (landed >> shift) ^ me
    local = landed & ((1 << shift) - 1)
    queue = planes * blocks

    rel_mine = rel[0, 0]
    mine = (rel_mine // inside)[None, :] == jnp.arange(planes, dtype=i32)[:, None]
    mine = jnp.pad(mine, ((0, 0), (0, queue - blocks)))
    column = rel[:, 0, :].reshape(1, queue)
    here = column < inside
    row_of = jnp.arange(queue, dtype=i32)[None, :] // blocks
    per_row = here & (row_of == jnp.arange(planes, dtype=i32)[:, None])
    to_dest = column == jnp.arange(inside, dtype=i32)[:, None]
    to_me = (rel == 0).transpose(1, 0, 2).reshape(inside, queue)
    local_of = local.transpose(1, 0, 2).reshape(inside, queue)
    ranks = earlier(jnp.concatenate([mine, per_row, to_dest, to_me], axis=0))
    rank_mine, rank_row, rank_dest, rank_me = jnp.split(
        ranks, [planes, 2 * planes, 2 * planes + inside]
    )
    rank_row = jnp.sum(jnp.where(per_row, rank_row, 0), axis=0, keepdims=True)

    wet = ocean_mask.reshape(tiles, cells)
    room1 = min(blocks, wide * cap)
    room2 = min(queue, planes * cap)
    slots = inside * room2
    index = jnp.arange(blocks, dtype=i32)
    src1 = pick(mine[:, :blocks], rank_mine[:, :blocks], room1, index).reshape(-1)
    src2 = pick(to_dest, rank_dest, room2, row_of * room1 + rank_row).reshape(-1)
    tile_of = pick(to_me, rank_me, room2, (local_of + 1)[:, None, :]).reshape(-1)
    slot = jnp.arange(slots, dtype=i32)
    alike = (tile_of[:, None] == tile_of[None, :]) & (slot[None, :] < slot[:, None])
    alike = alike & (tile_of[:, None] > 0)
    prev = jnp.min(jnp.where(alike, slots - 1 - slot[None, :], slots), axis=1)
    prev = jnp.where(prev == slots, slots, slots - 1 - prev)
    listed = jnp.arange(tiles, dtype=i32) + 1
    hit = listed[:, None] == tile_of[None, :]
    last = jnp.min(jnp.where(hit, slots - 1 - slot[None, :], slots), axis=1)
    last = jnp.where(last == slots, slots, slots - 1 - last)
    lists = jnp.concatenate([src1, src2, prev, last])

    mean1 = blocks // planes
    mean2 = max(1, queue // everyone)
    sizes = [(a,) * planes for a in (44, 48)] if planes != 4 else [
        (40, 44, 40, 44), (44, 40, 44, 40), (38, 50, 50, 38), (50, 38, 38, 50),
        (46, 46, 46, 46), (40, 56, 40, 56), (56, 40, 56, 40),
    ]
    depths = (42, 42, 44, 44, 44, 46, 46)
    rooms = [
        (tuple(min(room1, a * mean1 // 32) for a in size), min(room2, b * mean2 // 16))
        for size, b in list(zip(sizes, depths)) + [((52,) * planes, 48), ((56,) * planes, 48)]
    ] + [((room1,) * planes, room2)]

    source = jnp.arange(everyone, dtype=i32).reshape(planes, inside) ^ me
    plane_of = ((landed >> shift) // inside).reshape(1, everyone, blocks)
    target = jnp.arange(planes, dtype=i32)[:, None]
    load1 = jnp.sum((plane_of == target[:, :, None]).astype(i32), axis=2)
    load1 = jnp.where((source // inside).reshape(1, everyone) == target, 0, load1)
    by_column = rel.transpose(1, 0, 2).reshape(inside, 1, queue)
    owners = jnp.arange(everyone, dtype=i32)[None, :, None]
    load2 = jnp.sum((by_column == owners).astype(i32), axis=2)
    need1, need2 = jnp.zeros_like(load1), jnp.zeros_like(load2)
    for n, (size, b) in enumerate(rooms[:-1]):
        allowed = sum((target == p).astype(i32) * a for p, a in enumerate(size))
        need1 = need1 | ((load1 > allowed).astype(i32) << n)
        need2 = need2 | ((load2 > b).astype(i32) << n)
    rows = max(planes, inside)
    need = jnp.pad(need1, ((0, rows - planes), (0, 0))) | jnp.pad(
        need2, ((0, rows - inside), (0, 0))
    )
    full = lax.reduce(need, np.int32(0), lax.bitwise_or, (0, 1))
    choice, still = jnp.int32(0), jnp.int32(1)
    for n in range(len(rooms) - 1):
        still = still & (full >> n)
        choice = choice + still

    def run(n):
        shape = (bands, halves, planes, room1, room2, *rooms[n], chunks, tiles)
        return exchange(shape, 2 + n, lists, partial, covered, wet)

    return lax.switch(choice, [functools.partial(run, n) for n in range(len(rooms))])


def solution(mesh):
    in_specs = (
        P(None, ("band", "sub")),
        P(("band", "sub"), None, None),
        P(("band", "sub")),
        P(("band", "sub"), None),
        P(("band", "sub")),
        P(("band", "sub")),
    )
    out_specs = P(None, ("band", "sub"))
    return jax.shard_map(
        per_device, mesh=mesh, in_specs=in_specs, out_specs=out_specs, check_vma=False
    )
```

```python
import functools

import jax
import jax.numpy as jnp
import numpy as np
from jax import lax
from jax.experimental import pallas as pl
from jax.experimental.pallas import tpu as pltpu
from jax.sharding import PartitionSpec as P

cover_floor = 0.5
ROWS = 8
MESH = pl.DeviceIdType.MESH
f32, bf16, i32 = jnp.float32, jnp.bfloat16, jnp.int32


def peers_of(me, low, size):
    steps, bit = [], low
    while bit < size:
        steps.append(bit - 2 * bit * lax.rem(me // bit, 2))
        bit *= 2

    def peer(k):
        index = me
        for n, step in enumerate(steps):
            if not isinstance(k, int):
                index = index + step * lax.rem(k // 2 ** n, 2)
            elif k // 2 ** n % 2:
                index = index + step
        return index

    return peer


def block_kernel(
    group, chunks, bands, halves, tiles, shift,
    v_ref, w_ref, m_ref, band_ref, tile_ref, p_ref, c_ref, r_ref,
    values, weights, named, landed, v_sem, w_sem, send_sem, recv_sem,
):
    band = lax.axis_index("band")
    half = lax.axis_index("sub")
    blocks, cells, _ = weights.shape
    everyone = bands * halves
    pieces = blocks // group

    def value_copy(i):
        lanes = pl.ds(pl.multiple_of(i * group * cells, cells), group * cells)
        return pltpu.make_async_copy(v_ref.at[:, lanes], values.at[:, lanes], v_sem.at[i])

    def weight_copy(i):
        rows = pl.ds(i * group, group)
        return pltpu.make_async_copy(w_ref.at[rows], weights.at[rows], w_sem.at[i])

    for i in range(pieces):
        value_copy(i).start()
        weight_copy(i).start()

    band_at, half_at = peers_of(band, 1, bands), peers_of(half, 1, halves)

    def peer(k):
        return {"band": band_at(k // halves), "sub": half_at(k % halves)}

    def index_copy(k):
        return pltpu.make_async_remote_copy(
            src_ref=named, dst_ref=landed.at[k],
            send_sem=send_sem.at[k], recv_sem=recv_sem.at[k],
            device_id=peer(k), device_id_type=MESH,
        )

    barrier = pltpu.get_barrier_semaphore()
    for k in range(1, everyone):
        pl.semaphore_signal(barrier, inc=1, device_id=peer(k), device_id_type=MESH)

    tile = tile_ref[...]
    side = jnp.zeros_like(tile)
    for h in range(1, halves):
        side = side + (tile >= h * tiles).astype(i32)
    named[...] = (band_ref[...] * halves + side) * (1 << shift) + tile - side * tiles

    def multiply(i):
        value_copy(i).wait()
        weight_copy(i).wait()
        for u in range(group):
            j = i * group + u
            lanes = pl.ds(pl.multiple_of(j * cells, cells), cells)
            mb = m_ref[:, lanes].astype(f32).astype(bf16)
            lhs = jnp.concatenate(
                [values[:, lanes] * mb, jnp.broadcast_to(mb, (16, cells))], axis=0
            )
            p = jnp.dot(lhs, weights[j], preferred_element_type=f32)
            for c in range(chunks):
                p_ref[c, j] = p[c * ROWS:(c + 1) * ROWS].astype(bf16)
            c_ref[pl.ds(j, 1), :] = p[chunks * ROWS:chunks * ROWS + 1].astype(bf16).astype(f32)

    multiply(0)
    pl.semaphore_wait(barrier, everyone - 1)
    for k in range(1, everyone):
        index_copy(k).start()

    @pl.loop(1, pieces)
    def _(i):
        multiply(i)

    for k in range(1, everyone):
        index_copy(k).wait_send()
        index_copy(k).wait_recv()

    r_ref[0] = named[...]
    r_ref[pl.ds(1, everyone - 1)] = landed[pl.ds(1, everyone - 1)]


def block_products(bands, halves, tiles, shift, values, weights, mask, band, tile):
    fields = values.shape[0]
    blocks, cells, out_cells = weights.shape
    chunks = fields // ROWS
    group = 16
    pieces = blocks // group
    everyone = bands * halves
    vmem = pl.BlockSpec(memory_space=pltpu.VMEM)
    hbm = pl.BlockSpec(memory_space=pltpu.HBM)
    dma = pltpu.SemaphoreType.DMA
    return pl.pallas_call(
        functools.partial(block_kernel, group, chunks, bands, halves, tiles, shift),
        in_specs=[hbm, hbm, vmem, vmem, vmem],
        out_specs=[vmem, vmem, vmem],
        out_shape=[
            jax.ShapeDtypeStruct((chunks, blocks, ROWS, out_cells), bf16),
            jax.ShapeDtypeStruct((blocks, out_cells), f32),
            jax.ShapeDtypeStruct((everyone, 1, blocks), i32),
        ],
        scratch_shapes=[
            pltpu.VMEM(values.shape, bf16),
            pltpu.VMEM(weights.shape, bf16),
            pltpu.VMEM((1, blocks), i32),
            pltpu.VMEM((everyone, 1, blocks), i32),
            dma((pieces,)),
            dma((pieces,)),
            dma((everyone,)),
            dma((everyone,)),
        ],
        compiler_params=pltpu.CompilerParams(
            collective_id=1, has_side_effects=True, vmem_limit_bytes=59 * 1024 * 1024
        ),
        name="block_products",
    )(values, weights, mask, band, tile)


def exchange_kernel(
    shape, list_ref, p_ref, c_ref, wet_ref, out_ref, *scratch
):
    bands, halves, planes, room1, room2, firsts, second, chunks, tiles = shape
    first = max(firsts)
    wide = bands // planes
    inside = wide * halves
    cover1, cover2 = -(-first // 8) * 8, -(-second // 8) * 8
    slots = inside * room2
    send1, send2, recv2, run, done = scratch[:5]
    csend1, crecv1, cheld, csend2, crecv2, cstage, crun, factor = scratch[5:13]
    sem1, rem1, sem2, rem2, csem1, crem1, csem2, crem2, out_sem = scratch[13:22]
    recv1 = scratch[22:]
    band = lax.axis_index("band")
    half = lax.axis_index("sub")
    cells = c_ref.shape[1]
    at2 = planes * room1
    at_prev = at2 + slots
    at_last = at_prev + slots

    here = band // wide
    z_at = peers_of(here, 1, planes)
    wide_at, half_at = peers_of(band, 1, wide), peers_of(half, 1, halves)

    def z_peer(k):
        return {"band": band + (z_at(k) - here) * wide}

    def plane_peer(k):
        return {"band": wide_at(k // halves), "sub": half_at(k % halves)}

    barrier = pltpu.get_barrier_semaphore()

    @pl.loop(1, planes)
    def _(k):
        pl.semaphore_signal(barrier, inc=1, device_id=z_peer(k), device_id_type=MESH)

    @pl.loop(1, inside)
    def _(k):
        pl.semaphore_signal(barrier, inc=1, device_id=plane_peer(k), device_id_type=MESH)

    pl.semaphore_wait(barrier, planes + inside - 2)

    def z_copy(c, k, size):
        return pltpu.make_async_remote_copy(
            src_ref=send1.at[c, k, pl.ds(0, size)],
            dst_ref=recv1[c].at[pl.ds(k * room1, size)],
            send_sem=sem1.at[c, k], recv_sem=rem1.at[c, k],
            device_id=z_peer(k), device_id_type=MESH,
        )

    def each_target(body):
        for plane in range(planes):
            @pl.when(here != plane)
            def _(plane=plane):
                body(z_at(plane), firsts[plane])

    def each_source(body):
        for plane in range(planes):
            @pl.when(here == plane)
            def _(plane=plane):
                for k in range(1, planes):
                    body(k, firsts[plane])

    def plane_copy(c, k):
        return pltpu.make_async_remote_copy(
            src_ref=send2.at[c, k], dst_ref=recv2.at[c, k],
            send_sem=sem2.at[c, k], recv_sem=rem2.at[c, k],
            device_id=plane_peer(k), device_id_type=MESH,
        )

    def z_cover(k):
        return pltpu.make_async_remote_copy(
            src_ref=csend1.at[k], dst_ref=crecv1.at[k],
            send_sem=csem1.at[k], recv_sem=crem1.at[k],
            device_id=z_peer(k), device_id_type=MESH,
        )

    def plane_cover(k):
        return pltpu.make_async_remote_copy(
            src_ref=csend2.at[k], dst_ref=crecv2.at[k],
            send_sem=csem2.at[k], recv_sem=crem2.at[k],
            device_id=plane_peer(k), device_id_type=MESH,
        )

    def out_copy(c):
        return pltpu.make_async_copy(
            done.at[c % 2], out_ref.at[pl.ds(c * ROWS, ROWS), :], out_sem.at[c % 2]
        )

    def each(count, body, step=4):
        @pl.loop(0, count // step)
        def _(g):
            for u in range(step):
                body(g * step + u)

        for j in range(count // step * step, count):
            body(j)

    def send_chunk(c):
        def to_plane(k, size):
            def pack(j):
                send1[c, k, j] = p_ref[c, list_ref[k * room1 + j]]

            each(size, pack)
            z_copy(c, k, size).start()

        each_target(to_plane)

        def keep(j):
            recv1[c][j] = p_ref[c, list_ref[j]]

        each(room1, keep)

    def forward_chunk(c):
        @pl.loop(1, inside)
        def _(k):
            def pack(j):
                send2[c, k, j] = recv1[c][list_ref[at2 + k * room2 + j]]

            each(second, pack)
            plane_copy(c, k).start()

    def add_chunk(c):
        run[slots] = jnp.zeros((ROWS, cells), f32)

        def own_slot(j):
            run[j] = run[list_ref[at_prev + j]] + recv1[c][list_ref[at2 + j]].astype(f32)

        each(second, own_slot)

        @pl.loop(1, inside)
        def _(k):
            plane_copy(c, k).wait_recv()

            def one(j):
                i = k * room2 + j
                run[i] = run[list_ref[at_prev + i]] + recv2[c, k, j].astype(f32)

            each(second, one)

        if c >= 2:
            out_copy(c - 2).wait()

        def finish(t):
            lanes = pl.ds(pl.multiple_of(t * cells, cells), cells)
            done[c % 2, :, lanes] = run[list_ref[at_last + t]] * factor[pl.ds(t, 1), :]

        each(tiles, finish)
        out_copy(c).start()

    def send_covers():
        @pl.loop(1, planes)
        def _(k):
            def pack(j):
                cstage[pl.ds(j, 1), :] = c_ref[pl.ds(list_ref[k * room1 + j], 1), :]

            each(first, pack)
            csend1[k] = cstage[pl.ds(0, cover1), :].astype(bf16)
            z_cover(k).start()

        def keep(j):
            cheld[pl.ds(j, 1), :] = c_ref[pl.ds(list_ref[j], 1), :]

        each(room1, keep)

    def forward_covers():
        for k in range(1, planes):
            z_cover(k).wait_recv()
            cheld[pl.ds(k * room1, cover1), :] = crecv1[k].astype(f32)

        @pl.loop(1, inside)
        def _(k):
            def pack(j):
                cstage[pl.ds(j, 1), :] = cheld[pl.ds(list_ref[at2 + k * room2 + j], 1), :]

            each(second, pack)
            csend2[k] = cstage[pl.ds(0, cover2), :].astype(bf16)
            plane_cover(k).start()

    def add_covers():
        crun[pl.ds(slots, 8), :] = jnp.zeros((8, cells), f32)

        def own_slot(j):
            crun[pl.ds(j, 1), :] = (
                crun[pl.ds(list_ref[at_prev + j], 1), :]
                + cheld[pl.ds(list_ref[at2 + j], 1), :]
            )

        each(second, own_slot)

        @pl.loop(1, inside)
        def _(k):
            plane_cover(k).wait_recv()
            cstage[pl.ds(0, cover2), :] = crecv2[k].astype(f32)

            def one(j):
                i = k * room2 + j
                crun[pl.ds(i, 1), :] = (
                    crun[pl.ds(list_ref[at_prev + i], 1), :] + cstage[pl.ds(j, 1), :]
                )

            each(second, one)

        def total(t):
            factor[pl.ds(t, 1), :] = crun[pl.ds(list_ref[at_last + t], 1), :]

        each(tiles, total)
        factor[...] = wet_ref[...].astype(f32) / jnp.maximum(factor[...], cover_floor)

    window, lag = 2, 1
    cstage[...] = jnp.zeros_like(cstage)
    send_chunk(0)
    send_covers()
    for c in range(1, min(window, chunks)):
        send_chunk(c)

    for c in range(chunks):
        each_source(lambda k, size: z_copy(c, k, size).wait_recv())
        forward_chunk(c)
        if c + window < chunks:
            send_chunk(c + window)
        if c == 0:
            forward_covers()
        if c == lag:
            add_covers()
        if c >= lag:
            add_chunk(c - lag)

    for c in range(chunks - lag, chunks):
        add_chunk(c)

    @pl.loop(1, planes)
    def _(k):
        z_cover(k).wait_send()

    for c in range(chunks):
        each_target(lambda k, size: z_copy(c, k, size).wait_send())

    @pl.loop(1, inside)
    def _(k):
        plane_cover(k).wait_send()
        for c in range(chunks):
            plane_copy(c, k).wait_send()

    for c in range(chunks - 2, chunks):
        out_copy(c).wait()


def exchange(shape, ident, lists, partial, covered, wet):
    bands, halves, planes, room1, room2, firsts, second, chunks, tiles = shape
    first = max(firsts)
    _, _, rows, cells = partial.shape
    inside = bands * halves // planes
    slots = inside * room2
    cover1, cover2 = -(-first // 8) * 8, -(-second // 8) * 8
    smem = pl.BlockSpec(memory_space=pltpu.SMEM)
    vmem = pl.BlockSpec(memory_space=pltpu.VMEM)
    dma = pltpu.SemaphoreType.DMA
    return pl.pallas_call(
        functools.partial(exchange_kernel, shape),
        in_specs=[smem, vmem, vmem, vmem],
        out_specs=pl.BlockSpec(memory_space=pl.ANY),
        out_shape=jax.ShapeDtypeStruct((chunks * rows, tiles * cells), f32),
        scratch_shapes=[
            pltpu.VMEM((chunks, planes, first, rows, cells), bf16),
            pltpu.VMEM((chunks, inside, second, rows, cells), bf16),
            pltpu.VMEM((chunks, inside, second, rows, cells), bf16),
            pltpu.VMEM((slots + 1, rows, cells), f32),
            pltpu.VMEM((2, rows, tiles * cells), f32),
            pltpu.VMEM((planes, cover1, cells), bf16),
            pltpu.VMEM((planes, cover1, cells), bf16),
            pltpu.VMEM((planes * room1, cells), f32),
            pltpu.VMEM((inside, cover2, cells), bf16),
            pltpu.VMEM((inside, cover2, cells), bf16),
            pltpu.VMEM((max(cover1, cover2), cells), f32),
            pltpu.VMEM((slots + 8, cells), f32),
            pltpu.VMEM((tiles, cells), f32),
            dma((chunks, planes)),
            dma((chunks, planes)),
            dma((chunks, inside)),
            dma((chunks, inside)),
            dma((planes,)),
            dma((planes,)),
            dma((inside,)),
            dma((inside,)),
            dma((2,)),
        ] + [pltpu.VMEM((planes * room1, rows, cells), bf16) for _ in range(chunks)],
        compiler_params=pltpu.CompilerParams(
            collective_id=ident, has_side_effects=True, vmem_limit_bytes=40 * 1024 * 1024
        ),
        name="exchange",
    )(lists, partial, covered, wet)


def earlier(masks):
    size = masks.shape[1]
    order = jnp.arange(size, dtype=i32)
    before = (order[:, None] < order[None, :]).astype(bf16)
    return jnp.dot(masks.astype(bf16), before, preferred_element_type=f32).astype(i32)


def pick(masks, rank, room, values):
    slot = jnp.arange(room, dtype=i32)
    hit = masks[:, None, :] & (rank[:, None, :] == slot[None, :, None])
    return jnp.sum(jnp.where(hit, values, 0), axis=2)


def per_device(land_values, area_weights, land_mask, dest_band, dest_tile, ocean_mask):
    blocks = area_weights.shape[0]
    cells = area_weights.shape[2]
    chunks = land_values.shape[0] // ROWS
    bands = lax.axis_size("band")
    halves = lax.axis_size("sub")
    everyone = bands * halves
    me = lax.axis_index("band") * halves + lax.axis_index("sub")
    tiles = ocean_mask.shape[0] // cells
    cap = max(2, 2 * blocks // bands)
    planes = 2 ** ((bands.bit_length() - 1) // 2)
    wide = bands // planes
    inside = wide * halves
    shift = (tiles - 1).bit_length()

    partial, covered, landed = block_products(
        bands, halves, tiles, shift, land_values, area_weights,
        land_mask[None, :], dest_band.reshape(1, blocks), dest_tile[None, :],
    )

    landed = landed.reshape(planes, inside, blocks)
    rel = (landed >> shift) ^ me
    local = landed & ((1 << shift) - 1)
    queue = planes * blocks

    rel_mine = rel[0, 0]
    mine = (rel_mine // inside)[None, :] == jnp.arange(planes, dtype=i32)[:, None]
    mine = jnp.pad(mine, ((0, 0), (0, queue - blocks)))
    column = rel[:, 0, :].reshape(1, queue)
    here = column < inside
    row_of = jnp.arange(queue, dtype=i32)[None, :] // blocks
    per_row = here & (row_of == jnp.arange(planes, dtype=i32)[:, None])
    to_dest = column == jnp.arange(inside, dtype=i32)[:, None]
    to_me = (rel == 0).transpose(1, 0, 2).reshape(inside, queue)
    local_of = local.transpose(1, 0, 2).reshape(inside, queue)
    ranks = earlier(jnp.concatenate([mine, per_row, to_dest, to_me], axis=0))
    rank_mine, rank_row, rank_dest, rank_me = jnp.split(
        ranks, [planes, 2 * planes, 2 * planes + inside]
    )
    rank_row = jnp.sum(jnp.where(per_row, rank_row, 0), axis=0, keepdims=True)

    wet = ocean_mask.reshape(tiles, cells)
    room1 = min(blocks, wide * cap)
    room2 = min(queue, planes * cap)
    slots = inside * room2
    index = jnp.arange(blocks, dtype=i32)
    src1 = pick(mine[:, :blocks], rank_mine[:, :blocks], room1, index).reshape(-1)
    src2 = pick(to_dest, rank_dest, room2, row_of * room1 + rank_row).reshape(-1)
    tile_of = pick(to_me, rank_me, room2, (local_of + 1)[:, None, :]).reshape(-1)
    slot = jnp.arange(slots, dtype=i32)
    alike = (tile_of[:, None] == tile_of[None, :]) & (slot[None, :] < slot[:, None])
    alike = alike & (tile_of[:, None] > 0)
    prev = jnp.min(jnp.where(alike, slots - 1 - slot[None, :], slots), axis=1)
    prev = jnp.where(prev == slots, slots, slots - 1 - prev)
    listed = jnp.arange(tiles, dtype=i32) + 1
    hit = listed[:, None] == tile_of[None, :]
    last = jnp.min(jnp.where(hit, slots - 1 - slot[None, :], slots), axis=1)
    last = jnp.where(last == slots, slots, slots - 1 - last)
    lists = jnp.concatenate([src1, src2, prev, last])

    mean1 = blocks // planes
    mean2 = max(1, queue // everyone)
    sizes = [(a,) * planes for a in (44, 48)]
    depths = (44, 44)
    rooms = [
        (tuple(min(room1, a * mean1 // 32) for a in size), min(room2, b * mean2 // 16))
        for size, b in list(zip(sizes, depths)) + [((54,) * planes, 48)]
    ] + [((room1,) * planes, room2)]

    source = jnp.arange(everyone, dtype=i32).reshape(planes, inside) ^ me
    plane_of = ((landed >> shift) // inside).reshape(1, everyone, blocks)
    target = jnp.arange(planes, dtype=i32)[:, None]
    load1 = jnp.sum((plane_of == target[:, :, None]).astype(i32), axis=2)
    load1 = jnp.where((source // inside).reshape(1, everyone) == target, 0, load1)
    by_column = rel.transpose(1, 0, 2).reshape(inside, 1, queue)
    owners = jnp.arange(everyone, dtype=i32)[None, :, None]
    load2 = jnp.sum((by_column == owners).astype(i32), axis=2)
    need1, need2 = jnp.zeros_like(load1), jnp.zeros_like(load2)
    for n, (size, b) in enumerate(rooms[:-1]):
        allowed = sum((target == p).astype(i32) * a for p, a in enumerate(size))
        need1 = need1 | ((load1 > allowed).astype(i32) << n)
        need2 = need2 | ((load2 > b).astype(i32) << n)
    rows = max(planes, inside)
    need = jnp.pad(need1, ((0, rows - planes), (0, 0))) | jnp.pad(
        need2, ((0, rows - inside), (0, 0))
    )
    full = lax.reduce(need, np.int32(0), lax.bitwise_or, (0, 1))
    choice = lax.population_count((full ^ (full + 1)) >> 1)

    def run(n):
        shape = (bands, halves, planes, room1, room2, *rooms[n], chunks, tiles)
        return exchange(shape, 2 + n, lists, partial, covered, wet)

    return lax.switch(choice, [functools.partial(run, n) for n in range(len(rooms))])


def solution(mesh):
    in_specs = (
        P(None, ("band", "sub")),
        P(("band", "sub"), None, None),
        P(("band", "sub")),
        P(("band", "sub"), None),
        P(("band", "sub")),
        P(("band", "sub")),
    )
    out_specs = P(None, ("band", "sub"))
    return jax.shard_map(
        per_device, mesh=mesh, in_specs=in_specs, out_specs=out_specs, check_vma=False
    )
```
